32 devices in a mesh: phase: 2 (over x), slab: 8 (over z, y), arm: 2 (over core).
Axes of the slice: x: 2, y: 2, z: 4, core: 2. Of those that a mesh axis runs over, the one named last changes fastest.
Arguments:
- field_w: float32 [2, 64, 32, 128], P(None, ('phase', 'slab')), parts along dimension 1, may hold values from -0.6 to 0.6, as said below
- metric: float32 [12], P('phase'), parts along dimension 0, may hold values from -0.25 to 1, as said below
- arm_length: float32 [16], P('arm'), may hold values from 0.4 to 1
- arm_steps: int32 [16], P('arm'), may hold values from 8 to 16
- arm_species: int32 [16], P('arm'), may hold values from 0 to 1
Outputs:
- density: float32 [2, 64, 32, 128], P(None, ('phase', 'slab'), 'arm'), parts along dimension 1
- stress: float32 [12], P('phase'), parts along dimension 0
The draws below stay inside these ranges and needn't reach their ends.
There are 2 independent parts, one for each index of `phase`. The reference program is written for one: setup_inputs(seed, part) draws one part's arguments, and reference() takes and returns one part's arrays. A program takes and returns all parts, laid end to end along the dimension named above; an argument that names none is the same for every part. Nothing has to cross between parts.
Inputs may be any that keep to these rules, and one draw needn't show every extreme that they name: `field_w`: potentials of the two species at each cell. The first three entries are the diagonal of the inverse metric, from 0.7 to 1; the last three are its off-diagonal entries, from -0.25 to 0.25.
All inputs are finite; a program needn't handle non-finite values.
Results may differ from the reference program's by a relative error of at most 0.0003.
Values sent between devices are 32-bit elements; how exact they have to be, the bound alone decides.
No kernel may reach another device: no remote copies, remote signals or barrier semaphores. Data moves between devices by JAX's collectives and lax.ppermute only.
A program may use at most 64 MiB of HBM per device.

```python
import jax
import jax.numpy as jnp
from jax import lax

ARMS = 16
SPECIES = 2
STEPS = 16
CY = 32
CZ = 128
NX = 32


def draw_field_w(key, part):
    first_key = jax.random.fold_in(jax.random.fold_in(key, 11), 0)
    position = jnp.arange(NX, dtype=jnp.float32) / NX - 0.5
    rough = 0.15 * jnp.clip(jax.random.normal(first_key, (SPECIES, NX, CY, CZ), jnp.float32), -2.5, 2.5)
    slope = 0.12
    return rough + slope * position[None, :, None, None]


def draw_metric(key, part):
    first_key, second_key = jax.random.split(jax.random.fold_in(key, 23), 2)
    diagonal = jax.random.uniform(first_key, (3,), jnp.float32, 0.7, 1.0)
    coupled = jax.random.uniform(second_key, (3,), jnp.float32, -0.25, 0.25)
    return jnp.concatenate([diagonal, coupled])


def touch_ends(result, rng, low, high):
    extent = result.shape
    spot = [jax.random.randint(jax.random.fold_in(rng, axis), (), 0, extent[axis]) for axis in range(len(extent))]
    result = result.at[tuple(spot)].set(low)
    longest = extent.index(max(extent))
    spot[longest] = (spot[longest] + 1) % extent[longest]
    return result.at[tuple(spot)].set(high)


def block_levels(key, shape, pieces, least, top_value):
    def one(axis_at, shards_of):
        draws = jax.random.uniform(jax.random.fold_in(jax.random.fold_in(key, 6), axis_at), (shards_of,), jnp.float32, least / len(pieces), top_value / len(pieces))
        return jnp.repeat(jnp.exp(draws), shape[axis_at] // shards_of).reshape((-1,) + (1,) * (len(shape) - axis_at - 1))

    loudness = one(*pieces[0])
    for cut in pieces[1:]:
        loudness = loudness * one(*cut)
    return loudness


def setup_inputs(seed: int = 0, part: int = 0) -> dict:
    key_list = jax.random.split(jax.random.key(seed), 6)
    part_splits = jax.random.split(jax.random.fold_in(key_list[5], part), 6)
    return {
        "field_w": draw_field_w(jax.random.fold_in(jax.random.fold_in(key_list[5], part), 71), part),
        "metric": draw_metric(jax.random.fold_in(jax.random.fold_in(key_list[5], part), 71), part),
        "arm_length": jnp.clip(0.4 + 0.6 * jax.random.uniform(key_list[2], (ARMS,), jnp.float32) ** block_levels(key_list[2], (ARMS,), ((0, 2),), -0.2, 0.2), 0.4, 1.0),
        "arm_steps": touch_ends(jax.random.randint(key_list[3], (ARMS,), STEPS // 2, STEPS + 1), jax.random.fold_in(key_list[3], 1), STEPS // 2, STEPS).astype(jnp.int32),
        "arm_species": touch_ends(jax.random.randint(key_list[4], (ARMS,), 0, SPECIES), jax.random.fold_in(key_list[4], 1), 0, SPECIES - 1).astype(jnp.int32),
    }


def upward(values, along):
    return jnp.roll(values, -1, along)


def downward(values, along):
    return jnp.roll(values, 1, along)


def differences(centre, plus_x, minus_x):
    second_xx = plus_x + minus_x - 2.0 * centre
    second_yy = upward(centre, 2) + downward(centre, 2) - 2.0 * centre
    second_zz = upward(centre, 3) + downward(centre, 3) - 2.0 * centre
    second_xy = 0.25 * (upward(plus_x, 2) - downward(plus_x, 2) - upward(minus_x, 2) + downward(minus_x, 2))
    second_xz = 0.25 * (upward(plus_x, 3) - downward(plus_x, 3) - upward(minus_x, 3) + downward(minus_x, 3))
    above_y = upward(centre, 2)
    below_y = downward(centre, 2)
    second_yz = 0.25 * (upward(above_y, 3) - downward(above_y, 3) - upward(below_y, 3) + downward(below_y, 3))
    return (second_xx, second_yy, second_zz, second_xy, second_xz, second_yz)


def laplace(seconds, metric):
    diagonal_part = metric[0] * seconds[0] + metric[1] * seconds[1] + metric[2] * seconds[2]
    return diagonal_part + 2.0 * (metric[3] * seconds[3] + metric[4] * seconds[4] + metric[5] * seconds[5])


def advance(propagator, half_decay, step_size, metric, active):
    scaled = half_decay * propagator
    seconds = differences(scaled, jnp.roll(scaled, -1, 1), jnp.roll(scaled, 1, 1))
    updated = half_decay * (scaled + step_size[:, None, None, None] * laplace(seconds, metric))
    return jnp.where(active[:, None, None, None], updated, propagator), seconds


def species_mix(selector, fields):
    mixed_sum = selector[:, 0, None, None, None] * fields[0][None]
    for species in range(1, fields.shape[0]):
        mixed_sum = mixed_sum + selector[:, species, None, None, None] * fields[species][None]
    return mixed_sum


def gather_species(selector, per_arm):
    return jnp.stack([jnp.sum(selector[:, species, None, None, None] * per_arm, axis=0) for species in range(selector.shape[1])])


def exclusive_product(finals):
    lower = jnp.cumprod(finals, axis=0)
    upper = jnp.cumprod(finals[::-1], axis=0)[::-1]
    unity = jnp.ones_like(finals[:1])
    before = jnp.concatenate([unity, lower[:-1]], 0)
    after = jnp.concatenate([upper[1:], unity], 0)
    return before * after, lower[-1]


def contour_weight(position, arm_counts, step_size):
    ends = jnp.logical_or(position == 0, position == arm_counts)
    return step_size * jnp.where(position > arm_counts, 0.0, jnp.where(ends, 0.5, 1.0))


def reference(field_w, metric, arm_length, arm_steps, arm_species):
    step_size = arm_length / arm_steps.astype(jnp.float32)
    selector = (arm_species[:, None] == jnp.arange(SPECIES, dtype=jnp.int32)[None, :]).astype(jnp.float32)
    half_decay = jnp.exp(-0.5 * step_size[:, None, None, None] * species_mix(selector, field_w))
    propagator = jnp.ones(half_decay.shape, jnp.float32)
    history = [propagator]
    for step_index in range(STEPS):
        active = step_index >= STEPS - arm_steps
        propagator, unused = advance(propagator, half_decay, step_size, metric, active)
        history.append(propagator)
    adjoint, product_all = exclusive_product(propagator)
    density_acc = jnp.zeros(half_decay.shape, jnp.float32)
    stress_acc = jnp.zeros((6,), jnp.float32)
    for step_index in range(STEPS + 1):
        paired = history[STEPS - step_index]
        density_acc = density_acc + contour_weight(step_index, arm_steps, step_size)[:, None, None, None] * paired * adjoint
        if step_index < STEPS:
            active = step_index < arm_steps
            adjoint, seconds = advance(adjoint, half_decay, step_size, metric, active)
            arm_sums = jnp.stack([jnp.sum(paired * second, axis=(1, 2, 3)) for second in seconds])
            stress_acc = stress_acc + jnp.dot(arm_sums, step_size * active.astype(jnp.float32), precision=lax.Precision.HIGHEST)
    partition = jnp.sum(product_all)
    cell_count = NX * CY * CZ
    density_scale = cell_count / (ARMS * partition)
    density = gather_species(selector, density_acc) * density_scale
    stress = stress_acc / (ARMS * partition)
    return density, stress
```

```python
import functools

import jax
import jax.numpy as jnp
from jax import lax
from jax.experimental import pallas as pl
from jax.experimental.pallas import tpu as pltpu
from jax.sharding import PartitionSpec as P

STEPS = 16
ROWS = 8
PLANES = 8


def up_y(parts):
    return parts[1:] + [pltpu.roll(parts[0], ROWS - 1, 0)]


def down_y(parts):
    return [pltpu.roll(parts[-1], 1, 0)] + parts[:-1]


def up_z(value):
    return pltpu.roll(value, value.shape[1] - 1, 1)


def down_z(value):
    return pltpu.roll(value, 1, 1)


def splat(scalar, lanes):
    return jnp.full((ROWS, lanes), scalar, jnp.float32)


def coefficients(arm, lanes, length_ref, steps_ref, metric_ref):
    mu = splat(length_ref[arm], lanes) / splat(steps_ref[arm].astype(jnp.float32), lanes)
    return mu, [mu * metric_ref[k] for k in range(6)]


def blocks(planes):
    size = PLANES if planes % PLANES == 0 else 1
    return planes // size, size


def forward_kernel(arms, length_ref, steps_ref, metric_ref, field_ref, hist_ref, half_ref, keep_ref, give_ref):
    _, planes, parts, _, lanes = hist_ref.shape
    slabs, depth = field_ref.shape[:2]
    arm, core = lax.rem(lax.axis_index("slab"), arms), lax.axis_index("arm")
    count = steps_ref[arm]
    mu, scaled = coefficients(arm, lanes, length_ref, steps_ref, metric_ref)
    c_x, c_y, c_z = scaled[:3]
    c_xy, c_xz, c_yz = (0.5 * s for s in scaled[3:])
    c_0 = 1.0 - 2.0 * (c_x + c_y + c_z)
    decay = -0.5 * mu

    @pl.loop(0, slabs)
    def _(slab):
        for i in range(depth):
            for j in range(parts):
                value = field_ref[slab, i, pl.ds(j, ROWS, stride=parts), :]
                half_ref[slab * depth + i, j] = jnp.exp(decay * value)
                hist_ref[0, slab * depth + i, j] = jnp.ones((ROWS, lanes), jnp.float32)

    trips, size = blocks(planes)

    @pl.loop(0, count)
    def _(step):
        def plane(x):
            x = lax.rem(x, planes)
            half = [half_ref[x, j] for j in range(parts)]
            return half, [half[j] * hist_ref[step, x, j] for j in range(parts)]

        def block(trip, carry):
            minus, centre, half = carry
            first = trip * size
            for i in range(size):
                next_half, plus = plane(first + i + 1)
                diff = [p - m for p, m in zip(plus, minus)]
                total = [p + m for p, m in zip(plus, minus)]
                above, below = up_y(centre), down_y(centre)
                diff_above, diff_below = up_y(diff), down_y(diff)
                for j in range(parts):
                    skew = c_xz * diff[j] + c_yz * (above[j] - below[j])
                    main = c_z * centre[j]
                    value = (
                        c_0 * centre[j]
                        + c_x * total[j]
                        + c_y * (above[j] + below[j])
                        + c_xy * (diff_above[j] - diff_below[j])
                        + (up_z(main + skew) + down_z(main - skew))
                    )
                    hist_ref[step + 1, first + i, j] = half[j] * value
                minus, centre, half = centre, plus, next_half
            return minus, centre, half

        _, before = plane(planes - 1)
        half, here = plane(0)
        lax.fori_loop(0, trips, block, (before, here, half))

    split = parts // 2

    @pl.loop(0, planes)
    def _(x):
        for j in range(split):
            keep_ref[x, j] = hist_ref[count, x, core * split + j]
            give_ref[x, j] = hist_ref[count, x, (1 - core) * split + j]


def exclusive_kernel(arms, pairs_ref, out_ref):
    slabs, rows, _ = pairs_ref.shape

    @pl.loop(0, rows // ROWS)
    def _(block):
        at = pl.ds(pl.multiple_of(block * ROWS, ROWS), ROWS)
        values = [pairs_ref[a, at, :] for a in range(arms)]
        before, after = [None] * arms, [None] * arms
        for a in range(1, arms):
            before[a] = values[a - 1] if before[a - 1] is None else before[a - 1] * values[a - 1]
            b = arms - 1 - a
            after[b] = values[b + 1] if after[b + 1] is None else after[b + 1] * values[b + 1]
        for a in range(arms):
            sides = [s for s in (before[a], after[a]) if s is not None]
            result = sides[0] * sides[1] if len(sides) == 2 else sides[0]
            for copy in range(a, slabs, arms):
                out_ref[copy, at, :] = result


def adjoint_kernel(
    arms, length_ref, steps_ref, species_ref, metric_ref, hist_ref, half_ref, mine_ref, other_ref, out_ref,
    state_ref, square_ref, density_ref, line_ref, tail_ref,
):
    _, planes, parts, _, lanes = hist_ref.shape
    arm, core = lax.rem(lax.axis_index("slab"), arms), lax.axis_index("arm")
    count = steps_ref[arm]
    mu, scaled = coefficients(arm, lanes, length_ref, steps_ref, metric_ref)
    c_x, c_y, c_z = scaled[:3]
    c_xy, c_xz, c_yz = (0.5 * s for s in scaled[3:])
    c_0 = 1.0 - 2.0 * c_z
    split = parts // 2
    zero = jnp.zeros((ROWS, lanes), jnp.float32)

    def start(x, total):
        for j in range(split):
            for source, side in ((mine_ref, core), (other_ref, 1 - core)):
                at = side * split + j
                adjoint = source[x, j]
                half = half_ref[x, at]
                state = half * adjoint
                end = hist_ref[count, x, at]
                state_ref[0, x, at] = state
                square_ref[x, at] = half * half
                density_ref[x, at] = (-0.5 * end) * state
                total = total + end * adjoint
        return total

    partition = lax.fori_loop(0, planes, start, zero)
    trips, size = blocks(planes)

    def advance(step, sums):
        now, later = lax.rem(step, 2), lax.rem(step + 1, 2)

        def plane(x):
            x = lax.rem(x, planes)
            return [state_ref[now, x, j] for j in range(parts)]

        def block(trip, carry):
            minus, centre, sums = carry
            sums = list(sums)
            first = trip * size
            for i in range(size):
                x = first + i
                plus = plane(x + 1)
                diff = [p - m for p, m in zip(plus, minus)]
                total = [p + m for p, m in zip(plus, minus)]
                above, below = up_y(centre), down_y(centre)
                diff_above, diff_below = up_y(diff), down_y(diff)
                for j in range(parts):
                    paired = hist_ref[count - step, x, j]
                    twice = centre[j] + centre[j]
                    s_xx = total[j] - twice
                    s_yy = (above[j] + below[j]) - twice
                    d_xy = diff_above[j] - diff_below[j]
                    d_y = above[j] - below[j]
                    skew = c_xz * diff[j] + c_yz * d_y
                    main = c_z * centre[j]
                    value = (
                        c_0 * centre[j]
                        + c_x * s_xx
                        + c_y * s_yy
                        + c_xy * d_xy
                        + (up_z(main + skew) + down_z(main - skew))
                    )
                    state_ref[later, x, j] = square_ref[x, j] * value
                    paired_up, paired_down = up_z(paired), down_z(paired)
                    q_zz = (paired_up + paired_down) - (paired + paired)
                    q_z = paired_down - paired_up
                    density_ref[x, j] = density_ref[x, j] + paired * centre[j]
                    terms = (
                        paired * s_xx, paired * s_yy, q_zz * centre[j],
                        paired * d_xy, q_z * diff[j], q_z * d_y,
                    )
                    sums = [s + t for s, t in zip(sums, terms)]
                minus, centre = centre, plus
            return minus, centre, tuple(sums)

        return lax.fori_loop(0, trips, block, (plane(planes - 1), plane(0), sums))[2]

    sums = lax.fori_loop(0, count, advance, (zero,) * 6)
    last = lax.rem(count, 2)

    @pl.loop(0, planes)
    def _(x):
        for j in range(parts):
            final = 0.5 * (hist_ref[0, x, j] * state_ref[last, x, j])
            density = mu * (density_ref[x, j] + final) / half_ref[x, j]
            line_ref[x, pl.ds(j, ROWS, stride=parts), :] = density

    owners = out_ref.shape[0]
    cores = lax.axis_size("arm")
    depth, near = planes * cores // owners, line_ref.shape[1] // cores
    body = depth * near
    weights = (1.0, 1.0, 1.0, 0.25, 0.25, 0.25)
    for k in range(6):
        tail_ref[k : k + 1, :] = jnp.sum((weights[k] * mu) * sums[k], axis=0, keepdims=True)
    tail_ref[6:7, :] = jnp.sum(partition, axis=0, keepdims=True)
    tail_ref[7:8, :] = jnp.full((1, lanes), species_ref[arm].astype(jnp.float32), jnp.float32)

    @pl.loop(0, owners // cores)
    def _(slab):
        for side in range(cores):
            for i in range(depth):
                out_ref[slab * cores + side, i * near : (i + 1) * near, :] = line_ref[
                    slab * depth + i, side * near : (side + 1) * near, :
                ]
            out_ref[slab * cores + side, body : body + ROWS, :] = tail_ref[...]


def owner_kernel(arms, cores, cells, shares_ref, density_ref, stress_ref):
    species, depth, near, lanes = density_ref.shape
    body = depth * near
    senders = range(arms * cores)
    tails = [shares_ref[a, body : body + ROWS, :] for a in senders]
    total = tails[0]
    for a in senders[1:]:
        total = total + tails[a]
    partition = jnp.broadcast_to(jnp.sum(tails[0][6:7, :], axis=1, keepdims=True), (ROWS, lanes))
    norm = (arms * cores) * partition
    scale = cells / norm
    stress = total / norm
    for k in range(6):
        stress_ref[k] = jnp.sum(stress[k : k + 1, :])
    kinds = [jnp.broadcast_to(t[7:8, :], (ROWS, lanes)) for t in tails]
    for i in range(depth):
        for r in range(0, near, ROWS):
            values = [shares_ref[a, i * near + r : i * near + r + ROWS, :] for a in senders]
            for kind in range(species):
                picked = [jnp.where(kinds[a] == float(kind), values[a], 0.0) for a in senders]
                result = picked[0]
                for value in picked[1:]:
                    result = result + value
                density_ref[kind, i, r : r + ROWS, :] = result * scale


def local(field_w, metric, arm_length, arm_steps, arm_species):
    species, depth, rows, lanes = field_w.shape
    arms, slabs, cores = arm_length.shape[0], lax.axis_size("slab"), lax.axis_size("arm")
    assert slabs % arms == 0 and cores == 2 and rows % (2 * ROWS) == 0
    planes, parts = slabs * depth, rows // ROWS
    f32, vmem, smem = jnp.float32, pl.BlockSpec(memory_space=pltpu.VMEM), pl.BlockSpec(memory_space=pltpu.SMEM)
    params = pltpu.CompilerParams(vmem_limit_bytes=56 * 1024 * 1024)
    swap = [(0, 1), (1, 0)]

    wanted = jnp.tile(arm_species, slabs // arms)[:, None, None, None]
    chosen = jnp.broadcast_to(field_w[0][None], (slabs, depth, rows, lanes))
    for kind in range(1, species):
        chosen = jnp.where(wanted == kind, field_w[kind][None], chosen)
    field = lax.all_to_all(chosen, "slab", 0, 0, tiled=True)

    grid = (planes, parts, ROWS, lanes)
    piece = (planes, parts // 2, ROWS, lanes)
    hist, half, keep, give = pl.pallas_call(
        functools.partial(forward_kernel, arms),
        out_shape=[
            jax.ShapeDtypeStruct((STEPS + 1,) + grid, f32),
            jax.ShapeDtypeStruct(grid, f32),
            jax.ShapeDtypeStruct(piece, f32),
            jax.ShapeDtypeStruct(piece, f32),
        ],
        in_specs=[smem] * 3 + [vmem],
        out_specs=[vmem] * 4,
        compiler_params=params,
        name="forward",
    )(arm_length, arm_steps, metric, field)

    other = lax.ppermute(give, "arm", swap)
    flat = (slabs, depth * (parts // 2) * ROWS, lanes)
    pairs = lax.all_to_all((keep * other).reshape(flat), "slab", 0, 0, tiled=True)
    rest = pl.pallas_call(
        functools.partial(exclusive_kernel, arms),
        out_shape=jax.ShapeDtypeStruct(flat, f32),
        in_specs=[vmem],
        out_specs=vmem,
        name="exclusive",
    )(pairs)
    rest = lax.all_to_all(rest, "slab", 0, 0, tiled=True).reshape(piece)
    beyond = lax.ppermute(rest * keep, "arm", swap)

    body = depth * (rows // cores)
    shares = pl.pallas_call(
        functools.partial(adjoint_kernel, arms),
        out_shape=jax.ShapeDtypeStruct((slabs * cores, body + ROWS, lanes), f32),
        in_specs=[smem] * 4 + [vmem] * 4,
        out_specs=vmem,
        scratch_shapes=[
            pltpu.VMEM((2,) + grid, f32),
            pltpu.VMEM(grid, f32),
            pltpu.VMEM(grid, f32),
            pltpu.VMEM((planes, rows, lanes), f32),
            pltpu.VMEM((ROWS, lanes), f32),
        ],
        compiler_params=params,
        name="adjoint",
    )(arm_length, arm_steps, arm_species, metric, hist, half, rest * other, beyond)

    shares = lax.all_to_all(shares, ("slab", "arm"), 0, 0, tiled=True)
    cells = float(planes * rows * lanes)
    return pl.pallas_call(
        functools.partial(owner_kernel, arms, cores, cells),
        out_shape=[
            jax.ShapeDtypeStruct((species, depth, rows // cores, lanes), f32),
            jax.ShapeDtypeStruct((6,), f32),
        ],
        in_specs=[vmem],
        out_specs=[vmem, smem],
        name="owner",
    )(shares)


def solution(mesh):
    return jax.shard_map(
        local,
        mesh=mesh,
        in_specs=(P(None, ("phase", "slab"), None, None), P("phase"), P("arm"), P("arm"), P("arm")),
        out_specs=(P(None, ("phase", "slab"), "arm", None), P("phase")),
        check_vma=False,
    )
```

```python
import functools

import jax
import jax.numpy as jnp
from jax import lax
from jax.experimental import pallas as pl
from jax.experimental.pallas import tpu as pltpu
from jax.sharding import PartitionSpec as P

STEPS = 16
ROWS = 8


def up_y(parts):
    return parts[1:] + [pltpu.roll(parts[0], ROWS - 1, 0)]


def down_y(parts):
    return [pltpu.roll(parts[-1], 1, 0)] + parts[:-1]


def up_z(value):
    return pltpu.roll(value, value.shape[1] - 1, 1)


def down_z(value):
    return pltpu.roll(value, 1, 1)


def splat(scalar, lanes):
    return jnp.full((ROWS, lanes), scalar, jnp.float32)


def coefficients(arm, lanes, length_ref, steps_ref, metric_ref):
    mu = splat(length_ref[arm], lanes) / splat(steps_ref[arm].astype(jnp.float32), lanes)
    return mu, [mu * metric_ref[k] for k in range(3)] + [(0.5 * mu) * metric_ref[k] for k in range(3, 6)]


def put(state, x, j, value):
    value_ref, sum_ref, slope_ref = state
    above, below = up_z(value), down_z(value)
    value_ref[x, j] = value
    sum_ref[x, j] = above + below
    slope_ref[x, j] = above - below


def sweep(state, visit):
    value_ref, sum_ref, slope_ref = state
    planes, parts = value_ref.shape[:2]

    def plane(ref, x):
        return [ref[x % planes, j] for j in range(parts)]

    minus, centre = plane(value_ref, -1), plane(value_ref, 0)
    slope_minus, slope = plane(slope_ref, -1), plane(slope_ref, 0)
    for x in range(planes):
        plus, slope_plus = plane(value_ref, x + 1), plane(slope_ref, x + 1)
        diff = [p - m for p, m in zip(plus, minus)]
        above, below = up_y(centre), down_y(centre)
        for j in range(parts):
            visit(
                x, j, centre[j], plus[j] + minus[j], above[j] + below[j], sum_ref[x, j], diff,
                slope_plus[j] - slope_minus[j], slope,
            )
        minus, centre = centre, plus
        slope_minus, slope = slope, slope_plus


def in_pairs(count, step, first, second, carry):
    def both(k, carry):
        carry = step(2 * k, first, second, carry)
        return lax.cond(
            2 * k + 1 < count, lambda c: step(2 * k + 1, second, first, c), lambda c: c, carry
        )

    return lax.fori_loop(0, (count + 1) // 2, both, carry)


def forward_kernel(
    arms, length_ref, steps_ref, metric_ref, field_ref, hist_ref, half_ref, keep_ref, give_ref, *scratch
):
    _, planes, parts, _, lanes = hist_ref.shape
    slabs, depth = field_ref.shape[:2]
    arm, core = lax.rem(lax.axis_index("slab"), arms), lax.axis_index("arm")
    count = steps_ref[arm]
    mu, (c_x, c_y, c_z, c_xy, c_xz, c_yz) = coefficients(arm, lanes, length_ref, steps_ref, metric_ref)
    c_0 = 1.0 - 2.0 * (c_x + c_y + c_z)
    decay = -0.5 * mu
    first, second = scratch[:3], scratch[3:]

    for x in range(planes):
        for j in range(parts):
            half = jnp.exp(decay * field_ref[x // depth, x % depth, pl.ds(j, ROWS, stride=parts), :])
            half_ref[x, j] = half
            put(first, x, j, half)

    def step(k, source, target, carry):
        def visit(x, j, centre, sum_x, sum_y, sum_z, diff, slope_x, slope):
            if j == 0:
                skew = [c_xy * d + c_yz * s for d, s in zip(diff, slope)]
                visit.skew = [a - b for a, b in zip(up_y(skew), down_y(skew))]
            value = (
                (c_0 * centre + c_x * sum_x) + (c_y * sum_y + c_z * sum_z) + (c_xz * slope_x + visit.skew[j])
            )
            half = half_ref[x, j]
            value = half * value
            hist_ref[k, x, j] = value
            put(target, x, j, half * value)

        sweep(source, visit)
        return carry

    in_pairs(count, step, first, second, 0)
    split = parts // 2
    for x in range(planes):
        for j in range(split):
            keep_ref[x, j] = hist_ref[count - 1, x, core * split + j]
            give_ref[x, j] = hist_ref[count - 1, x, (1 - core) * split + j]


def exclusive_kernel(arms, pairs_ref, out_ref):
    slabs, rows, _ = pairs_ref.shape

    @pl.loop(0, rows // ROWS)
    def _(block):
        at = pl.ds(pl.multiple_of(block * ROWS, ROWS), ROWS)
        values = [pairs_ref[a, at, :] for a in range(arms)]
        before, after = [None] * arms, [None] * arms
        for a in range(1, arms):
            before[a] = values[a - 1] if before[a - 1] is None else before[a - 1] * values[a - 1]
            b = arms - 1 - a
            after[b] = values[b + 1] if after[b + 1] is None else after[b + 1] * values[b + 1]
        for a in range(arms):
            sides = [s for s in (before[a], after[a]) if s is not None]
            result = sides[0] * sides[1] if len(sides) == 2 else sides[0]
            for copy in range(a, slabs, arms):
                out_ref[copy, at, :] = result


def adjoint_kernel(
    arms, length_ref, steps_ref, species_ref, metric_ref, hist_ref, half_ref, mine_ref, other_ref, out_ref,
    square_ref, density_ref, line_ref, tail_ref, *scratch,
):
    _, planes, parts, _, lanes = hist_ref.shape
    arm, core = lax.rem(lax.axis_index("slab"), arms), lax.axis_index("arm")
    count = steps_ref[arm]
    mu, (c_x, c_y, c_z, c_xy, c_xz, c_yz) = coefficients(arm, lanes, length_ref, steps_ref, metric_ref)
    first, second = scratch[:3], scratch[3:]
    split = parts // 2
    zero = jnp.zeros((ROWS, lanes), jnp.float32)

    partition = zero
    for x in range(planes):
        for j in range(split):
            for source, side in ((mine_ref, core), (other_ref, 1 - core)):
                at = side * split + j
                adjoint = source[x, j]
                half = half_ref[x, at]
                value = half * adjoint
                end = hist_ref[count - 1, x, at]
                put(first, x, at, value)
                square_ref[x, at] = half * half
                density_ref[x, at] = (-0.5 * end) * value
                partition = partition + end * adjoint

    def step(k, source, target, sums):
        sums = list(sums)

        def visit(x, j, centre, sum_x, sum_y, sum_z, diff, slope_x, slope):
            if j == 0:
                visit.d_xy = [a - b for a, b in zip(up_y(diff), down_y(diff))]
                visit.d_yz = [a - b for a, b in zip(up_y(slope), down_y(slope))]
            twice = centre + centre
            s_xx, s_yy, s_zz = sum_x - twice, sum_y - twice, sum_z - twice
            s_xy, s_yz = visit.d_xy[j], visit.d_yz[j]
            value = (
                (centre + c_x * s_xx) + (c_y * s_yy + c_z * s_zz)
                + (c_xz * slope_x + (c_xy * s_xy + c_yz * s_yz))
            )
            put(target, x, j, square_ref[x, j] * value)
            paired = hist_ref[count - 1 - k, x, j]
            density_ref[x, j] = density_ref[x, j] + paired * centre
            for i, term in enumerate((s_xx, s_yy, s_zz, s_xy, slope_x, s_yz)):
                sums[i] = sums[i] + paired * term

        sweep(source, visit)
        return tuple(sums)

    sums = in_pairs(count, step, first, second, (zero,) * 6)

    def finish(value_ref):
        for x in range(planes):
            for j in range(parts):
                density = density_ref[x, j] + 0.5 * value_ref[x, j]
                line_ref[x, pl.ds(j, ROWS, stride=parts), :] = mu * density / half_ref[x, j]

    even = lax.rem(count, 2) == 0
    pl.when(even)(lambda: finish(first[0]))
    pl.when(jnp.logical_not(even))(lambda: finish(second[0]))

    owners = out_ref.shape[0]
    cores = lax.axis_size("arm")
    depth, near = planes * cores // owners, line_ref.shape[1] // cores
    body = depth * near
    weights = (1.0, 1.0, 1.0, 0.25, 0.25, 0.25)
    for k in range(6):
        tail_ref[k : k + 1, :] = jnp.sum((weights[k] * mu) * sums[k], axis=0, keepdims=True)
    tail_ref[6:7, :] = jnp.sum(partition, axis=0, keepdims=True)
    tail_ref[7:8, :] = jnp.full((1, lanes), species_ref[arm].astype(jnp.float32), jnp.float32)

    @pl.loop(0, owners // cores)
    def _(slab):
        for side in range(cores):
            for i in range(depth):
                out_ref[slab * cores + side, i * near : (i + 1) * near, :] = line_ref[
                    slab * depth + i, side * near : (side + 1) * near, :
                ]
            out_ref[slab * cores + side, body : body + ROWS, :] = tail_ref[...]


def owner_kernel(arms, cores, cells, shares_ref, density_ref, stress_ref):
    species, depth, near, lanes = density_ref.shape
    body = depth * near
    senders = range(arms * cores)
    tails = [shares_ref[a, body : body + ROWS, :] for a in senders]
    total = tails[0]
    for a in senders[1:]:
        total = total + tails[a]
    partition = jnp.broadcast_to(jnp.sum(tails[0][6:7, :], axis=1, keepdims=True), (ROWS, lanes))
    norm = (arms * cores) * partition
    scale = cells / norm
    stress = total / norm
    for k in range(6):
        stress_ref[k] = jnp.sum(stress[k : k + 1, :])
    kinds = [jnp.broadcast_to(t[7:8, :], (ROWS, lanes)) for t in tails]
    for i in range(depth):
        for r in range(0, near, ROWS):
            values = [shares_ref[a, i * near + r : i * near + r + ROWS, :] for a in senders]
            for kind in range(species):
                picked = [jnp.where(kinds[a] == float(kind), values[a], 0.0) for a in senders]
                result = picked[0]
                for value in picked[1:]:
                    result = result + value
                density_ref[kind, i, r : r + ROWS, :] = result * scale


def local(field_w, metric, arm_length, arm_steps, arm_species):
    species, depth, rows, lanes = field_w.shape
    arms, slabs, cores = arm_length.shape[0], lax.axis_size("slab"), lax.axis_size("arm")
    assert slabs % arms == 0 and cores == 2 and rows % (2 * ROWS) == 0
    planes, parts = slabs * depth, rows // ROWS
    f32, vmem, smem = jnp.float32, pl.BlockSpec(memory_space=pltpu.VMEM), pl.BlockSpec(memory_space=pltpu.SMEM)
    size = 4 * planes * rows * lanes
    params = pltpu.CompilerParams(vmem_limit_bytes=(STEPS + 16) * size)
    small = pltpu.CompilerParams(vmem_limit_bytes=8 * size)
    swap = [(0, 1), (1, 0)]

    wanted = jnp.tile(arm_species, slabs // arms)[:, None, None, None]
    chosen = jnp.broadcast_to(field_w[0][None], (slabs, depth, rows, lanes))
    for kind in range(1, species):
        chosen = jnp.where(wanted == kind, field_w[kind][None], chosen)
    field = lax.all_to_all(chosen, "slab", 0, 0, tiled=True)

    grid = (planes, parts, ROWS, lanes)
    piece = (planes, parts // 2, ROWS, lanes)
    hist, half, keep, give = pl.pallas_call(
        functools.partial(forward_kernel, arms),
        out_shape=[
            jax.ShapeDtypeStruct((STEPS,) + grid, f32),
            jax.ShapeDtypeStruct(grid, f32),
            jax.ShapeDtypeStruct(piece, f32),
            jax.ShapeDtypeStruct(piece, f32),
        ],
        in_specs=[smem] * 3 + [vmem],
        out_specs=[vmem] * 4,
        scratch_shapes=[pltpu.VMEM(grid, f32)] * 6,
        compiler_params=params,
        name="forward",
    )(arm_length, arm_steps, metric, field)

    other = lax.ppermute(give, "arm", swap)
    flat = (slabs, depth * (parts // 2) * ROWS, lanes)
    pairs = lax.all_to_all((keep * other).reshape(flat), "slab", 0, 0, tiled=True)
    rest = pl.pallas_call(
        functools.partial(exclusive_kernel, arms),
        out_shape=jax.ShapeDtypeStruct(flat, f32),
        in_specs=[vmem],
        out_specs=vmem,
        compiler_params=small,
        name="exclusive",
    )(pairs)
    rest = lax.all_to_all(rest, "slab", 0, 0, tiled=True).reshape(piece)
    beyond = lax.ppermute(rest * keep, "arm", swap)

    body = depth * (rows // cores)
    shares = pl.pallas_call(
        functools.partial(adjoint_kernel, arms),
        out_shape=jax.ShapeDtypeStruct((slabs * cores, body + ROWS, lanes), f32),
        in_specs=[smem] * 4 + [vmem] * 4,
        out_specs=vmem,
        scratch_shapes=[
            pltpu.VMEM(grid, f32),
            pltpu.VMEM(grid, f32),
            pltpu.VMEM((planes, rows, lanes), f32),
            pltpu.VMEM((ROWS, lanes), f32),
        ]
        + [pltpu.VMEM(grid, f32)] * 6,
        compiler_params=params,
        name="adjoint",
    )(arm_length, arm_steps, arm_species, metric, hist, half, rest * other, beyond)

    shares = lax.all_to_all(shares, ("slab", "arm"), 0, 0, tiled=True)
    cells = float(planes * rows * lanes)
    return pl.pallas_call(
        functools.partial(owner_kernel, arms, cores, cells),
        out_shape=[
            jax.ShapeDtypeStruct((species, depth, rows // cores, lanes), f32),
            jax.ShapeDtypeStruct((6,), f32),
        ],
        in_specs=[vmem],
        out_specs=[vmem, smem],
        compiler_params=small,
        name="owner",
    )(shares)


def solution(mesh):
    return jax.shard_map(
        local,
        mesh=mesh,
        in_specs=(P(None, ("phase", "slab"), None, None), P("phase"), P("arm"), P("arm"), P("arm")),
        out_specs=(P(None, ("phase", "slab"), "arm", None), P("phase")),
        check_vma=False,
    )
```

```python
import functools

import jax
import jax.numpy as jnp
from jax import lax
from jax.experimental import pallas as pl
from jax.experimental.pallas import tpu as pltpu
from jax.sharding import PartitionSpec as P

STEPS = 16
ROWS = 8


def up_y(parts):
    return parts[1:] + [pltpu.roll(parts[0], ROWS - 1, 0)]


def down_y(parts):
    return [pltpu.roll(parts[-1], 1, 0)] + parts[:-1]


def up_z(value):
    return pltpu.roll(value, value.shape[1] - 1, 1)


def down_z(value):
    return pltpu.roll(value, 1, 1)


def splat(scalar, lanes):
    return jnp.full((ROWS, lanes), scalar, jnp.float32)


MU, COUNT, SPECIES, METRIC = 0, 1, 2, 3


def prepare_kernel(*refs):
    sources, (chosen_ref, table_ref), targets, sems = refs[:5], refs[5:7], refs[7:12], refs[12]
    copies = [pltpu.make_async_copy(s, t, sems.at[i]) for i, (s, t) in enumerate(zip(sources, targets))]
    for copy in copies:
        copy.start()
    for copy in copies:
        copy.wait()
    length_ref, steps_ref, species_ref, metric_ref, field_ref = targets
    arms, (slabs, lanes) = length_ref.shape[0], (chosen_ref.shape[0], table_ref.shape[2])
    arm = lax.rem(lax.axis_index("slab"), arms)
    steps = splat(steps_ref[arm].astype(jnp.float32), lanes)
    mu = splat(length_ref[arm], lanes) / steps
    table_ref[MU] = mu
    table_ref[COUNT] = steps
    table_ref[SPECIES] = splat(species_ref[arm].astype(jnp.float32), lanes)
    for k in range(6):
        table_ref[METRIC + k] = (mu if k < 3 else 0.5 * mu) * metric_ref[k]
    for slab in range(slabs):
        chosen_ref[slab] = field_ref[species_ref[slab % arms]]


def unpack(table_ref):
    count = table_ref[COUNT][0, 0].astype(jnp.int32)
    return count, table_ref[MU], [table_ref[METRIC + k] for k in range(6)]


def put(state, x, j, value):
    value_ref, sum_ref, slope_ref = state
    above, below = up_z(value), down_z(value)
    value_ref[x, j] = value
    sum_ref[x, j] = above + below
    slope_ref[x, j] = above - below


def sweep(state, visit):
    value_ref, sum_ref, slope_ref = state
    planes, parts = value_ref.shape[:2]

    def plane(ref, x):
        return [ref[x % planes, j] for j in range(parts)]

    minus, centre = plane(value_ref, -1), plane(value_ref, 0)
    slope_minus, slope = plane(slope_ref, -1), plane(slope_ref, 0)
    for x in range(planes):
        plus, slope_plus = plane(value_ref, x + 1), plane(slope_ref, x + 1)
        diff = [p - m for p, m in zip(plus, minus)]
        above, below = up_y(centre), down_y(centre)
        for j in range(parts):
            visit(
                x, j, centre[j], plus[j] + minus[j], above[j] + below[j], sum_ref[x, j], diff,
                slope_plus[j] - slope_minus[j], slope,
            )
        minus, centre = centre, plus
        slope_minus, slope = slope, slope_plus


def in_pairs(count, step, first, second, carry):
    def both(k, carry):
        carry = step(2 * k, first, second, carry)
        return lax.cond(
            2 * k + 1 < count, lambda c: step(2 * k + 1, second, first, c), lambda c: c, carry
        )

    return lax.fori_loop(0, (count + 1) // 2, both, carry)


def forward_kernel(table_ref, field_ref, hist_ref, half_ref, keep_ref, give_ref, gain_ref, *scratch):
    planes, parts = half_ref.shape[:2]
    depth = field_ref.shape[1]
    core = lax.axis_index("arm")
    count, mu, (c_x, c_y, c_z, c_xy, c_xz, c_yz) = unpack(table_ref)
    c_0 = 1.0 - 2.0 * (c_x + c_y + c_z)
    c_0, c_y, c_z, c_xy, c_xz, c_yz = (c / c_x for c in (c_0, c_y, c_z, c_xy, c_xz, c_yz))
    decay = -0.5 * mu
    first, second = scratch[:3], scratch[3:]

    for x in range(planes):
        for j in range(parts):
            half = jnp.exp(decay * field_ref[x // depth, x % depth, pl.ds(j, ROWS, stride=parts), :])
            half_ref[x, j] = half
            gain_ref[x, j] = c_x * half
            put(first, x, j, half)

    def step(k, source, target, carry):
        def visit(x, j, centre, sum_x, sum_y, sum_z, diff, slope_x, slope):
            if j == 0:
                skew = [c_xy * d + c_yz * s for d, s in zip(diff, slope)]
                visit.skew = [a - b for a, b in zip(up_y(skew), down_y(skew))]
            value = (
                (c_0 * centre + sum_x) + (c_y * sum_y + c_z * sum_z) + (c_xz * slope_x + visit.skew[j])
            )
            value = gain_ref[x, j] * value
            hist_ref[k, x, j] = value
            put(target, x, j, half_ref[x, j] * value)

        sweep(source, visit)
        return carry

    in_pairs(count, step, first, second, 0)
    split = parts // 2
    for x in range(planes):
        for j in range(split):
            keep_ref[x, j] = hist_ref[count - 1, x, core * split + j]
            give_ref[x, j] = hist_ref[count - 1, x, (1 - core) * split + j]


def exclusive_kernel(arms, pairs_ref, out_ref):
    slabs, rows, _ = pairs_ref.shape

    @pl.loop(0, rows // ROWS)
    def _(block):
        at = pl.ds(pl.multiple_of(block * ROWS, ROWS), ROWS)
        values = [pairs_ref[a, at, :] for a in range(arms)]
        before, after = [None] * arms, [None] * arms
        for a in range(1, arms):
            before[a] = values[a - 1] if before[a - 1] is None else before[a - 1] * values[a - 1]
            b = arms - 1 - a
            after[b] = values[b + 1] if after[b + 1] is None else after[b + 1] * values[b + 1]
        for a in range(arms):
            sides = [s for s in (before[a], after[a]) if s is not None]
            result = sides[0] * sides[1] if len(sides) == 2 else sides[0]
            for copy in range(a, slabs, arms):
                out_ref[copy, at, :] = result


def adjoint_kernel(
    table_ref, hist_ref, half_ref, mine_ref, other_ref, out_ref, square_ref, density_ref, line_ref, tail_ref, *scratch
):
    planes, parts, _, lanes = half_ref.shape
    core = lax.axis_index("arm")
    count, mu, (c_x, c_y, c_z, c_xy, c_xz, c_yz) = unpack(table_ref)
    first, second = scratch[:3], scratch[3:]
    split = parts // 2
    zero = jnp.zeros((ROWS, lanes), jnp.float32)

    partition = zero
    for x in range(planes):
        for j in range(split):
            for source, side in ((mine_ref, core), (other_ref, 1 - core)):
                at = side * split + j
                adjoint = source[x, j]
                half = half_ref[x, at]
                value = half * adjoint
                end = hist_ref[count - 1, x, at]
                put(first, x, at, value)
                square_ref[x, at] = half * half
                density_ref[x, at] = (-0.5 * end) * value
                partition = partition + end * adjoint

    def step(k, source, target, sums):
        sums = list(sums)

        def visit(x, j, centre, sum_x, sum_y, sum_z, diff, slope_x, slope):
            if j == 0:
                visit.d_xy = [a - b for a, b in zip(up_y(diff), down_y(diff))]
                visit.d_yz = [a - b for a, b in zip(up_y(slope), down_y(slope))]
            twice = centre + centre
            s_xx, s_yy, s_zz = sum_x - twice, sum_y - twice, sum_z - twice
            s_xy, s_yz = visit.d_xy[j], visit.d_yz[j]
            value = (
                (centre + c_x * s_xx) + (c_y * s_yy + c_z * s_zz)
                + (c_xz * slope_x + (c_xy * s_xy + c_yz * s_yz))
            )
            put(target, x, j, square_ref[x, j] * value)
            paired = hist_ref[count - 1 - k, x, j]
            density_ref[x, j] = density_ref[x, j] + paired * centre
            for i, term in enumerate((s_xx, s_yy, s_zz, s_xy, slope_x, s_yz)):
                sums[i] = sums[i] + paired * term

        sweep(source, visit)
        return tuple(sums)

    sums = in_pairs(count, step, first, second, (zero,) * 6)

    def finish(value_ref):
        for x in range(planes):
            for j in range(parts):
                density = density_ref[x, j] + 0.5 * value_ref[x, j]
                line_ref[x, pl.ds(j, ROWS, stride=parts), :] = mu * density / half_ref[x, j]

    even = lax.rem(count, 2) == 0
    pl.when(even)(lambda: finish(first[0]))
    pl.when(jnp.logical_not(even))(lambda: finish(second[0]))

    owners = out_ref.shape[0]
    cores = lax.axis_size("arm")
    depth, near = planes * cores // owners, line_ref.shape[1] // cores
    body = depth * near
    weights = (1.0, 1.0, 1.0, 0.25, 0.25, 0.25)
    for k in range(6):
        tail_ref[k : k + 1, :] = jnp.sum((weights[k] * mu) * sums[k], axis=0, keepdims=True)
    tail_ref[6:7, :] = jnp.sum(partition, axis=0, keepdims=True)
    tail_ref[7:8, :] = table_ref[SPECIES, 0:1, :]

    @pl.loop(0, owners // cores)
    def _(slab):
        for side in range(cores):
            for i in range(depth):
                out_ref[slab * cores + side, i * near : (i + 1) * near, :] = line_ref[
                    slab * depth + i, side * near : (side + 1) * near, :
                ]
            out_ref[slab * cores + side, body : body + ROWS, :] = tail_ref[...]


def owner_kernel(arms, cores, cells, shares_ref, density_ref, stress_ref):
    species, depth, near, lanes = density_ref.shape
    body = depth * near
    senders = range(arms * cores)
    tails = [shares_ref[a, body : body + ROWS, :] for a in senders]
    total = tails[0]
    for a in senders[1:]:
        total = total + tails[a]
    partition = jnp.broadcast_to(jnp.sum(tails[0][6:7, :], axis=1, keepdims=True), (ROWS, lanes))
    norm = (arms * cores) * partition
    scale = cells / norm
    stress = total / norm
    for k in range(6):
        stress_ref[k] = jnp.sum(stress[k : k + 1, :])
    kinds = [jnp.broadcast_to(t[7:8, :], (ROWS, lanes)) for t in tails]
    for i in range(depth):
        for r in range(0, near, ROWS):
            values = [shares_ref[a, i * near + r : i * near + r + ROWS, :] for a in senders]
            for kind in range(species):
                picked = [jnp.where(kinds[a] == float(kind), values[a], 0.0) for a in senders]
                result = picked[0]
                for value in picked[1:]:
                    result = result + value
                density_ref[kind, i, r : r + ROWS, :] = result * scale


def local(field_w, metric, arm_length, arm_steps, arm_species):
    species, depth, rows, lanes = field_w.shape
    arms, slabs, cores = arm_length.shape[0], lax.axis_size("slab"), lax.axis_size("arm")
    assert slabs % arms == 0 and cores == 2 and rows % (2 * ROWS) == 0
    planes, parts = slabs * depth, rows // ROWS
    f32, vmem, smem = jnp.float32, pl.BlockSpec(memory_space=pltpu.VMEM), pl.BlockSpec(memory_space=pltpu.SMEM)
    size = 4 * planes * rows * lanes
    params = pltpu.CompilerParams(vmem_limit_bytes=(STEPS + 16) * size)
    small = pltpu.CompilerParams(vmem_limit_bytes=8 * size)
    swap = [(0, 1), (1, 0)]

    arguments = (arm_length, arm_steps, arm_species, metric, field_w)
    chosen, table = pl.pallas_call(
        prepare_kernel,
        out_shape=[
            jax.ShapeDtypeStruct((slabs, depth, rows, lanes), f32),
            jax.ShapeDtypeStruct((METRIC + 6, ROWS, lanes), f32),
        ],
        in_specs=[pl.BlockSpec(memory_space=pltpu.HBM)] * 5,
        out_specs=[vmem] * 2,
        scratch_shapes=[pltpu.SMEM(a.shape, a.dtype) for a in arguments[:4]]
        + [pltpu.VMEM(field_w.shape, f32), pltpu.SemaphoreType.DMA((5,))],
        compiler_params=small,
        name="prepare",
    )(*(pltpu.with_memory_space_constraint(a, pltpu.HBM) for a in arguments))
    field = lax.all_to_all(chosen, "slab", 0, 0, tiled=True)

    grid = (planes, parts, ROWS, lanes)
    piece = (planes, parts // 2, ROWS, lanes)
    hist, half, keep, give = pl.pallas_call(
        forward_kernel,
        out_shape=[
            jax.ShapeDtypeStruct((STEPS,) + grid, f32),
            jax.ShapeDtypeStruct(grid, f32),
            jax.ShapeDtypeStruct(piece, f32),
            jax.ShapeDtypeStruct(piece, f32),
        ],
        in_specs=[vmem] * 2,
        out_specs=[vmem] * 4,
        scratch_shapes=[pltpu.VMEM(grid, f32)] * 7,
        compiler_params=params,
        name="forward",
    )(table, field)

    other = lax.ppermute(give, "arm", swap)
    flat = (slabs, depth * (parts // 2) * ROWS, lanes)
    pairs = lax.all_to_all((keep * other).reshape(flat), "slab", 0, 0, tiled=True)
    rest = pl.pallas_call(
        functools.partial(exclusive_kernel, arms),
        out_shape=jax.ShapeDtypeStruct(flat, f32),
        in_specs=[vmem],
        out_specs=vmem,
        compiler_params=small,
        name="exclusive",
    )(pairs)
    rest = lax.all_to_all(rest, "slab", 0, 0, tiled=True).reshape(piece)
    beyond = lax.ppermute(rest * keep, "arm", swap)

    body = depth * (rows // cores)
    shares = pl.pallas_call(
        adjoint_kernel,
        out_shape=jax.ShapeDtypeStruct((slabs * cores, body + ROWS, lanes), f32),
        in_specs=[vmem] * 5,
        out_specs=vmem,
        scratch_shapes=[
            pltpu.VMEM(grid, f32),
            pltpu.VMEM(grid, f32),
            pltpu.VMEM((planes, rows, lanes), f32),
            pltpu.VMEM((ROWS, lanes), f32),
        ]
        + [pltpu.VMEM(grid, f32)] * 6,
        compiler_params=params,
        name="adjoint",
    )(table, hist, half, rest * other, beyond)

    shares = lax.all_to_all(shares, ("slab", "arm"), 0, 0, tiled=True)
    cells = float(planes * rows * lanes)
    return pl.pallas_call(
        functools.partial(owner_kernel, arms, cores, cells),
        out_shape=[
            jax.ShapeDtypeStruct((species, depth, rows // cores, lanes), f32),
            jax.ShapeDtypeStruct((6,), f32),
        ],
        in_specs=[vmem],
        out_specs=[vmem, smem],
        compiler_params=small,
        name="owner",
    )(shares)


def solution(mesh):
    return jax.shard_map(
        local,
        mesh=mesh,
        in_specs=(P(None, ("phase", "slab"), None, None), P("phase"), P("arm"), P("arm"), P("arm")),
        out_specs=(P(None, ("phase", "slab"), "arm", None), P("phase")),
        check_vma=False,
    )
```

```python
import functools

import jax
import jax.numpy as jnp
from jax import lax
from jax.experimental import pallas as pl
from jax.experimental.pallas import tpu as pltpu
from jax.sharding import PartitionSpec as P

STEPS = 16
ROWS = 8


def up_y(parts):
    return parts[1:] + [pltpu.roll(parts[0], ROWS - 1, 0)]


def down_y(parts):
    return [pltpu.roll(parts[-1], 1, 0)] + parts[:-1]


def up_z(value):
    return pltpu.roll(value, value.shape[1] - 1, 1)


def down_z(value):
    return pltpu.roll(value, 1, 1)


def splat(scalar, lanes):
    return jnp.full((ROWS, lanes), scalar, jnp.float32)


MU, COUNT, SPECIES, METRIC = 0, 1, 2, 3


def prepare_kernel(*refs):
    sources, (chosen_ref, table_ref), targets, sems = refs[:5], refs[5:7], refs[7:12], refs[12]
    copies = [pltpu.make_async_copy(s, t, sems.at[i]) for i, (s, t) in enumerate(zip(sources, targets))]
    for copy in copies:
        copy.start()
    for copy in copies:
        copy.wait()
    length_ref, steps_ref, species_ref, metric_ref, field_ref = targets
    arms, (slabs, lanes) = length_ref.shape[0], (chosen_ref.shape[0], table_ref.shape[2])
    arm = lax.rem(lax.axis_index("slab"), arms)
    steps = splat(steps_ref[arm].astype(jnp.float32), lanes)
    mu = splat(length_ref[arm], lanes) / steps
    table_ref[MU] = mu
    table_ref[COUNT] = steps
    table_ref[SPECIES] = splat(species_ref[arm].astype(jnp.float32), lanes)
    for k in range(6):
        table_ref[METRIC + k] = (mu if k < 3 else 0.5 * mu) * metric_ref[k]
    for slab in range(slabs):
        chosen_ref[slab] = field_ref[species_ref[slab % arms]]


def unpack(table_ref):
    count = table_ref[COUNT][0, 0].astype(jnp.int32)
    return count, table_ref[MU], [table_ref[METRIC + k] for k in range(6)]


def put(state, x, j, value):
    value_ref, sum_ref, slope_ref = state
    above, below = up_z(value), down_z(value)
    value_ref[x, j] = value
    sum_ref[x, j] = above + below
    slope_ref[x, j] = above - below


def sweep(state, visit):
    value_ref, sum_ref, slope_ref = state
    planes, parts = value_ref.shape[:2]

    def plane(ref, x):
        return [ref[x % planes, j] for j in range(parts)]

    minus, centre = plane(value_ref, -1), plane(value_ref, 0)
    slope_minus, slope = plane(slope_ref, -1), plane(slope_ref, 0)
    for x in range(planes):
        plus, slope_plus = plane(value_ref, x + 1), plane(slope_ref, x + 1)
        diff = [p - m for p, m in zip(plus, minus)]
        above, below = up_y(centre), down_y(centre)
        for j in range(parts):
            visit(
                x, j, centre[j], plus[j] + minus[j], above[j] + below[j], sum_ref[x, j], diff,
                slope_plus[j] - slope_minus[j], slope,
            )
        minus, centre = centre, plus
        slope_minus, slope = slope, slope_plus


def in_pairs(count, step, first, second):
    lone = lax.rem(count, 2)
    pl.when(lone == 1)(lambda: step(0, second, first))

    @pl.loop(0, count // 2)
    def _(pair):
        step(lone + 2 * pair, first, second)
        step(lone + 2 * pair + 1, second, first)


def forward_kernel(table_ref, field_ref, hist_ref, half_ref, keep_ref, give_ref, gain_ref, *scratch):
    planes, parts = half_ref.shape[:2]
    depth = field_ref.shape[1]
    core = lax.axis_index("arm")
    count, mu, (c_x, c_y, c_z, c_xy, c_xz, c_yz) = unpack(table_ref)
    c_0 = 1.0 - 2.0 * (c_x + c_y + c_z)
    c_0, c_y, c_z, c_xy, c_xz, c_yz = (c / c_x for c in (c_0, c_y, c_z, c_xy, c_xz, c_yz))
    decay = -0.5 * mu
    start, first, second = (tuple(r.at[at] for r in scratch) for at in (lax.rem(count, 2), 0, 1))

    for x in range(planes):
        for j in range(parts):
            half = jnp.exp(decay * field_ref[x // depth, x % depth, pl.ds(j, ROWS, stride=parts), :])
            half_ref[x, j] = half
            gain_ref[x, j] = c_x * half
            put(start, x, j, half)

    def step(k, source, target):
        def visit(x, j, centre, sum_x, sum_y, sum_z, diff, slope_x, slope):
            if j == 0:
                skew = [c_xy * d + c_yz * s for d, s in zip(diff, slope)]
                visit.skew = [a - b for a, b in zip(up_y(skew), down_y(skew))]
            value = (
                (c_0 * centre + sum_x) + (c_y * sum_y + c_z * sum_z) + (c_xz * slope_x + visit.skew[j])
            )
            value = gain_ref[x, j] * value
            hist_ref[k, x, j] = value
            put(target, x, j, half_ref[x, j] * value)

        sweep(source, visit)

    in_pairs(count, step, first, second)
    split = parts // 2
    for x in range(planes):
        for j in range(split):
            keep_ref[x, j] = hist_ref[count - 1, x, core * split + j]
            give_ref[x, j] = hist_ref[count - 1, x, (1 - core) * split + j]


def exclusive_kernel(arms, pairs_ref, out_ref):
    slabs, rows, _ = pairs_ref.shape

    @pl.loop(0, rows // ROWS)
    def _(block):
        at = pl.ds(pl.multiple_of(block * ROWS, ROWS), ROWS)
        values = [pairs_ref[a, at, :] for a in range(arms)]
        before, after = [None] * arms, [None] * arms
        for a in range(1, arms):
            before[a] = values[a - 1] if before[a - 1] is None else before[a - 1] * values[a - 1]
            b = arms - 1 - a
            after[b] = values[b + 1] if after[b + 1] is None else after[b + 1] * values[b + 1]
        for a in range(arms):
            sides = [s for s in (before[a], after[a]) if s is not None]
            result = sides[0] * sides[1] if len(sides) == 2 else sides[0]
            for copy in range(a, slabs, arms):
                out_ref[copy, at, :] = result


def adjoint_kernel(
    table_ref, hist_ref, half_ref, mine_ref, other_ref, out_ref, square_ref, density_ref, line_ref, tail_ref,
    total_ref, *scratch
):
    planes, parts, _, lanes = half_ref.shape
    core = lax.axis_index("arm")
    count, mu, (c_x, c_y, c_z, c_xy, c_xz, c_yz) = unpack(table_ref)
    start, first, second = (tuple(r.at[at] for r in scratch) for at in (lax.rem(count, 2), 0, 1))
    split = parts // 2
    zero = jnp.zeros((ROWS, lanes), jnp.float32)

    partition = zero
    for x in range(planes):
        for j in range(split):
            for source, side in ((mine_ref, core), (other_ref, 1 - core)):
                at = side * split + j
                adjoint = source[x, j]
                half = half_ref[x, at]
                value = half * adjoint
                end = hist_ref[count - 1, x, at]
                put(start, x, at, value)
                square_ref[x, at] = half * half
                density_ref[x, at] = (-0.5 * end) * value
                partition = partition + end * adjoint

    def step(k, source, target):
        sums = [total_ref[i] for i in range(6)]

        def visit(x, j, centre, sum_x, sum_y, sum_z, diff, slope_x, slope):
            if j == 0:
                visit.d_xy = [a - b for a, b in zip(up_y(diff), down_y(diff))]
                visit.d_yz = [a - b for a, b in zip(up_y(slope), down_y(slope))]
            twice = centre + centre
            s_xx, s_yy, s_zz = sum_x - twice, sum_y - twice, sum_z - twice
            s_xy, s_yz = visit.d_xy[j], visit.d_yz[j]
            value = (
                (centre + c_x * s_xx) + (c_y * s_yy + c_z * s_zz)
                + (c_xz * slope_x + (c_xy * s_xy + c_yz * s_yz))
            )
            put(target, x, j, square_ref[x, j] * value)
            paired = hist_ref[count - 1 - k, x, j]
            density_ref[x, j] = density_ref[x, j] + paired * centre
            for i, term in enumerate((s_xx, s_yy, s_zz, s_xy, slope_x, s_yz)):
                sums[i] = sums[i] + paired * term

        sweep(source, visit)
        for i in range(6):
            total_ref[i] = sums[i]

    for i in range(6):
        total_ref[i] = zero
    in_pairs(count, step, first, second)
    sums = [total_ref[i] for i in range(6)]

    for x in range(planes):
        for j in range(parts):
            density = density_ref[x, j] + 0.5 * first[0][x, j]
            line_ref[x, pl.ds(j, ROWS, stride=parts), :] = mu * density / half_ref[x, j]

    owners = out_ref.shape[0]
    cores = lax.axis_size("arm")
    depth, near = planes * cores // owners, line_ref.shape[1] // cores
    body = depth * near
    weights = (1.0, 1.0, 1.0, 0.25, 0.25, 0.25)
    for k in range(6):
        tail_ref[k : k + 1, :] = jnp.sum((weights[k] * mu) * sums[k], axis=0, keepdims=True)
    tail_ref[6:7, :] = jnp.sum(partition, axis=0, keepdims=True)
    tail_ref[7:8, :] = table_ref[SPECIES, 0:1, :]

    @pl.loop(0, owners // cores)
    def _(slab):
        for side in range(cores):
            for i in range(depth):
                out_ref[slab * cores + side, i * near : (i + 1) * near, :] = line_ref[
                    slab * depth + i, side * near : (side + 1) * near, :
                ]
            out_ref[slab * cores + side, body : body + ROWS, :] = tail_ref[...]


def owner_kernel(arms, cores, cells, shares_ref, density_ref, stress_ref):
    species, depth, near, lanes = density_ref.shape
    body = depth * near
    senders = range(arms * cores)
    tails = [shares_ref[a, body : body + ROWS, :] for a in senders]
    total = tails[0]
    for a in senders[1:]:
        total = total + tails[a]
    partition = jnp.broadcast_to(jnp.sum(tails[0][6:7, :], axis=1, keepdims=True), (ROWS, lanes))
    norm = (arms * cores) * partition
    scale = cells / norm
    stress = total / norm
    for k in range(6):
        stress_ref[k] = jnp.sum(stress[k : k + 1, :])
    kinds = [jnp.broadcast_to(t[7:8, :], (ROWS, lanes)) for t in tails]
    for i in range(depth):
        for r in range(0, near, ROWS):
            values = [shares_ref[a, i * near + r : i * near + r + ROWS, :] for a in senders]
            for kind in range(species):
                picked = [jnp.where(kinds[a] == float(kind), values[a], 0.0) for a in senders]
                result = picked[0]
                for value in picked[1:]:
                    result = result + value
                density_ref[kind, i, r : r + ROWS, :] = result * scale


def local(field_w, metric, arm_length, arm_steps, arm_species):
    species, depth, rows, lanes = field_w.shape
    arms, slabs, cores = arm_length.shape[0], lax.axis_size("slab"), lax.axis_size("arm")
    assert slabs % arms == 0 and cores == 2 and rows % (2 * ROWS) == 0
    planes, parts = slabs * depth, rows // ROWS
    f32, vmem, smem = jnp.float32, pl.BlockSpec(memory_space=pltpu.VMEM), pl.BlockSpec(memory_space=pltpu.SMEM)
    size = 4 * planes * rows * lanes
    params = pltpu.CompilerParams(vmem_limit_bytes=(STEPS + 16) * size)
    small = pltpu.CompilerParams(vmem_limit_bytes=8 * size)
    swap = [(0, 1), (1, 0)]

    arguments = (arm_length, arm_steps, arm_species, metric, field_w)
    chosen, table = pl.pallas_call(
        prepare_kernel,
        out_shape=[
            jax.ShapeDtypeStruct((slabs, depth, rows, lanes), f32),
            jax.ShapeDtypeStruct((METRIC + 6, ROWS, lanes), f32),
        ],
        in_specs=[pl.BlockSpec(memory_space=pltpu.HBM)] * 5,
        out_specs=[vmem] * 2,
        scratch_shapes=[pltpu.SMEM(a.shape, a.dtype) for a in arguments[:4]]
        + [pltpu.VMEM(field_w.shape, f32), pltpu.SemaphoreType.DMA((5,))],
        compiler_params=small,
        name="prepare",
    )(*(pltpu.with_memory_space_constraint(a, pltpu.HBM) for a in arguments))
    field = lax.all_to_all(chosen, "slab", 0, 0, tiled=True)

    grid = (planes, parts, ROWS, lanes)
    piece = (planes, parts // 2, ROWS, lanes)
    hist, half, keep, give = pl.pallas_call(
        forward_kernel,
        out_shape=[
            jax.ShapeDtypeStruct((STEPS,) + grid, f32),
            jax.ShapeDtypeStruct(grid, f32),
            jax.ShapeDtypeStruct(piece, f32),
            jax.ShapeDtypeStruct(piece, f32),
        ],
        in_specs=[vmem] * 2,
        out_specs=[vmem] * 4,
        scratch_shapes=[pltpu.VMEM(grid, f32)] + [pltpu.VMEM((2,) + grid, f32)] * 3,
        compiler_params=params,
        name="forward",
    )(table, field)

    other = lax.ppermute(give, "arm", swap)
    flat = (slabs, depth * (parts // 2) * ROWS, lanes)
    pairs = lax.all_to_all((keep * other).reshape(flat), "slab", 0, 0, tiled=True)
    rest = pl.pallas_call(
        functools.partial(exclusive_kernel, arms),
        out_shape=jax.ShapeDtypeStruct(flat, f32),
        in_specs=[vmem],
        out_specs=vmem,
        compiler_params=small,
        name="exclusive",
    )(pairs)
    rest = lax.all_to_all(rest, "slab", 0, 0, tiled=True).reshape(piece)
    beyond = lax.ppermute(rest * keep, "arm", swap)

    body = depth * (rows // cores)
    shares = pl.pallas_call(
        adjoint_kernel,
        out_shape=jax.ShapeDtypeStruct((slabs * cores, body + ROWS, lanes), f32),
        in_specs=[vmem] * 5,
        out_specs=vmem,
        scratch_shapes=[
            pltpu.VMEM(grid, f32),
            pltpu.VMEM(grid, f32),
            pltpu.VMEM((planes, rows, lanes), f32),
            pltpu.VMEM((ROWS, lanes), f32),
            pltpu.VMEM((6, ROWS, lanes), f32),
        ]
        + [pltpu.VMEM((2,) + grid, f32)] * 3,
        compiler_params=params,
        name="adjoint",
    )(table, hist, half, rest * other, beyond)

    shares = lax.all_to_all(shares, ("slab", "arm"), 0, 0, tiled=True)
    cells = float(planes * rows * lanes)
    return pl.pallas_call(
        functools.partial(owner_kernel, arms, cores, cells),
        out_shape=[
            jax.ShapeDtypeStruct((species, depth, rows // cores, lanes), f32),
            jax.ShapeDtypeStruct((6,), f32),
        ],
        in_specs=[vmem],
        out_specs=[vmem, smem],
        compiler_params=small,
        name="owner",
    )(shares)


def solution(mesh):
    return jax.shard_map(
        local,
        mesh=mesh,
        in_specs=(P(None, ("phase", "slab"), None, None), P("phase"), P("arm"), P("arm"), P("arm")),
        out_specs=(P(None, ("phase", "slab"), "arm", None), P("phase")),
        check_vma=False,
    )
```

```python
import functools

import jax
import jax.numpy as jnp
from jax import lax
from jax.experimental import pallas as pl
from jax.experimental.pallas import tpu as pltpu
from jax.sharding import PartitionSpec as P

STEPS = 16

ROWS = 8


def up_y(parts):
    return parts[1:] + [pltpu.roll(parts[0], ROWS - 1, 0)]


def down_y(parts):
    return [pltpu.roll(parts[-1], 1, 0)] + parts[:-1]


def up_z(value):
    return pltpu.roll(value, value.shape[1] - 1, 1)


def down_z(value):
    return pltpu.roll(value, 1, 1)


def splat(scalar, lanes):
    return jnp.full((ROWS, lanes), scalar, jnp.float32)


MU, COUNT, SPECIES, METRIC = 0, 1, 2, 3


def prepare_kernel(*refs):
    sources, (chosen_ref, table_ref), targets, sems = refs[:5], refs[5:7], refs[7:12], refs[12]
    copies = [pltpu.make_async_copy(s, t, sems.at[i]) for i, (s, t) in enumerate(zip(sources, targets))]
    for copy in copies:
        copy.start()
    for copy in copies:
        copy.wait()
    length_ref, steps_ref, species_ref, metric_ref, field_ref = targets
    arms, lanes = length_ref.shape[0], table_ref.shape[2]
    arm = lax.rem(lax.axis_index("slab"), arms)
    steps = splat(steps_ref[arm].astype(jnp.float32), lanes)
    mu = splat(length_ref[arm], lanes) / steps
    table_ref[MU] = mu
    table_ref[COUNT] = steps
    table_ref[SPECIES] = splat(species_ref[arm].astype(jnp.float32), lanes)
    for k in range(6):
        table_ref[METRIC + k] = (mu if k < 3 else 0.5 * mu) * metric_ref[k]
    chosen_ref[...] = field_ref[lax.axis_index("arm")]


def unpack(table_ref):
    count = table_ref[COUNT][0, 0].astype(jnp.int32)
    return count, table_ref[MU], [table_ref[METRIC + k] for k in range(6)]


def put(state, x, j, value):
    value_ref, sum_ref, slope_ref = state
    above, below = up_z(value), down_z(value)
    value_ref[x, j] = value
    sum_ref[x, j] = above + below
    slope_ref[x, j] = above - below


def sweep(state, visit):
    value_ref, sum_ref, slope_ref = state
    planes, parts = value_ref.shape[:2]

    def plane(ref, x):
        return [ref[x % planes, j] for j in range(parts)]

    minus, centre = plane(value_ref, -1), plane(value_ref, 0)
    slope_minus, slope = plane(slope_ref, -1), plane(slope_ref, 0)
    for x in range(planes):
        plus, slope_plus = plane(value_ref, x + 1), plane(slope_ref, x + 1)
        diff = [p - m for p, m in zip(plus, minus)]
        above, below = up_y(centre), down_y(centre)
        for j in range(parts):
            visit(
                x, j, centre[j], plus[j] + minus[j], above[j] + below[j], sum_ref[x, j], diff,
                slope_plus[j] - slope_minus[j], slope,
            )
        minus, centre = centre, plus
        slope_minus, slope = slope, slope_plus


def in_pairs(count, step, first, second):
    lone = lax.rem(count, 2)
    pl.when(lone == 1)(lambda: step(0, second, first))

    @pl.loop(0, count // 2)
    def _(pair):
        step(lone + 2 * pair, first, second)
        step(lone + 2 * pair + 1, second, first)


def forward_kernel(blocks, table_ref, other_ref, *refs):
    own_refs = refs[:blocks]
    hist_ref, half_ref, keep_ref, give_ref, gain_ref, *scratch = refs[blocks:]
    planes, parts = half_ref.shape[:2]
    depth = own_refs[0].shape[0]
    core = lax.axis_index("arm")
    count, mu, (c_x, c_y, c_z, c_xy, c_xz, c_yz) = unpack(table_ref)
    c_0 = 1.0 - 2.0 * (c_x + c_y + c_z)
    c_0, c_y, c_z, c_xy, c_xz, c_yz = (c / c_x for c in (c_0, c_y, c_z, c_xy, c_xz, c_yz))
    decay = -0.5 * mu
    start, first, second = (tuple(r.at[at] for r in scratch) for at in (lax.rem(count, 2), 0, 1))

    def begin(block_ref, block):
        base = (lax.axis_index("slab") ^ block) * depth
        for i in range(depth):
            for j in range(parts):
                half = jnp.exp(decay * block_ref[i, pl.ds(j, ROWS, stride=parts), :])
                half_ref[base + i, j] = half
                gain_ref[base + i, j] = c_x * half
                put(start, base + i, j, half)

    mine = table_ref[SPECIES][0, 0].astype(jnp.int32) == core

    @pl.when(mine)
    def _():
        for block in range(blocks):
            begin(own_refs[block], block)

    @pl.when(jnp.logical_not(mine))
    def _():
        for block in range(blocks):
            begin(other_ref.at[block], block)

    def step(k, source, target):
        def visit(x, j, centre, sum_x, sum_y, sum_z, diff, slope_x, slope):
            if j == 0:
                skew = [c_xy * d + c_yz * s for d, s in zip(diff, slope)]
                visit.skew = [a - b for a, b in zip(up_y(skew), down_y(skew))]
            value = (
                (c_0 * centre + sum_x) + (c_y * sum_y + c_z * sum_z) + (c_xz * slope_x + visit.skew[j])
            )
            value = gain_ref[x, j] * value
            hist_ref[k, x, j] = value
            put(target, x, j, half_ref[x, j] * value)

        sweep(source, visit)

    in_pairs(count, step, first, second)
    split = parts // 2
    for x in range(planes):
        for j in range(split):
            keep_ref[x, j] = hist_ref[count - 1, x, core * split + j]
            give_ref[x, j] = hist_ref[count - 1, x, (1 - core) * split + j]


def exclusive_kernel(arms, pairs_ref, out_ref):
    slabs, rows, _ = pairs_ref.shape

    @pl.loop(0, rows // ROWS)
    def _(block):
        at = pl.ds(pl.multiple_of(block * ROWS, ROWS), ROWS)
        values = [pairs_ref[a, at, :] for a in range(arms)]
        before, after = [None] * arms, [None] * arms
        for a in range(1, arms):
            before[a] = values[a - 1] if before[a - 1] is None else before[a - 1] * values[a - 1]
            b = arms - 1 - a
            after[b] = values[b + 1] if after[b + 1] is None else after[b + 1] * values[b + 1]
        for a in range(arms):
            sides = [s for s in (before[a], after[a]) if s is not None]
            result = sides[0] * sides[1] if len(sides) == 2 else sides[0]
            for copy in range(a, slabs, arms):
                out_ref[copy, at, :] = result


def adjoint_kernel(
    table_ref, hist_ref, half_ref, mine_ref, other_ref, out_ref, square_ref, density_ref, line_ref, tail_ref,
    total_ref, *scratch
):
    planes, parts, _, lanes = half_ref.shape
    core = lax.axis_index("arm")
    count, mu, (c_x, c_y, c_z, c_xy, c_xz, c_yz) = unpack(table_ref)
    start, first, second = (tuple(r.at[at] for r in scratch) for at in (lax.rem(count, 2), 0, 1))
    split = parts // 2
    zero = jnp.zeros((ROWS, lanes), jnp.float32)

    partition = zero
    for x in range(planes):
        for j in range(split):
            for source, side in ((mine_ref, core), (other_ref, 1 - core)):
                at = side * split + j
                adjoint = source[x, j]
                half = half_ref[x, at]
                value = half * adjoint
                end = hist_ref[count - 1, x, at]
                put(start, x, at, value)
                square_ref[x, at] = half * half
                density_ref[x, at] = (-0.5 * end) * value
                partition = partition + end * adjoint

    def step(k, source, target):
        sums = [total_ref[i] for i in range(6)]

        def visit(x, j, centre, sum_x, sum_y, sum_z, diff, slope_x, slope):
            if j == 0:
                visit.d_xy = [a - b for a, b in zip(up_y(diff), down_y(diff))]
                visit.d_yz = [a - b for a, b in zip(up_y(slope), down_y(slope))]
            twice = centre + centre
            s_xx, s_yy, s_zz = sum_x - twice, sum_y - twice, sum_z - twice
            s_xy, s_yz = visit.d_xy[j], visit.d_yz[j]
            value = (
                (centre + c_x * s_xx) + (c_y * s_yy + c_z * s_zz)
                + (c_xz * slope_x + (c_xy * s_xy + c_yz * s_yz))
            )
            put(target, x, j, square_ref[x, j] * value)
            paired = hist_ref[count - 1 - k, x, j]
            density_ref[x, j] = density_ref[x, j] + paired * centre
            for i, term in enumerate((s_xx, s_yy, s_zz, s_xy, slope_x, s_yz)):
                sums[i] = sums[i] + paired * term

        sweep(source, visit)
        for i in range(6):
            total_ref[i] = sums[i]

    for i in range(6):
        total_ref[i] = zero
    in_pairs(count, step, first, second)
    sums = [total_ref[i] for i in range(6)]

    for x in range(planes):
        for j in range(parts):
            density = density_ref[x, j] + 0.5 * first[0][x, j]
            line_ref[x, pl.ds(j, ROWS, stride=parts), :] = mu * density / half_ref[x, j]

    owners = out_ref.shape[0]
    cores = lax.axis_size("arm")
    depth, near = planes * cores // owners, line_ref.shape[1] // cores
    body = depth * near
    weights = (1.0, 1.0, 1.0, 0.25, 0.25, 0.25)
    for k in range(6):
        tail_ref[k : k + 1, :] = jnp.sum((weights[k] * mu) * sums[k], axis=0, keepdims=True)
    tail_ref[6:7, :] = jnp.sum(partition, axis=0, keepdims=True)
    tail_ref[7:8, :] = table_ref[SPECIES, 0:1, :]

    @pl.loop(0, owners // cores)
    def _(slab):
        for side in range(cores):
            for i in range(depth):
                out_ref[slab * cores + side, i * near : (i + 1) * near, :] = line_ref[
                    slab * depth + i, side * near : (side + 1) * near, :
                ]
            out_ref[slab * cores + side, body : body + ROWS, :] = tail_ref[...]


def owner_kernel(arms, cores, cells, shares_ref, density_ref, stress_ref):
    species, depth, near, lanes = density_ref.shape
    body = depth * near
    senders = range(arms * cores)
    tails = [shares_ref[a, body : body + ROWS, :] for a in senders]
    total = tails[0]
    for a in senders[1:]:
        total = total + tails[a]
    partition = jnp.broadcast_to(jnp.sum(tails[0][6:7, :], axis=1, keepdims=True), (ROWS, lanes))
    norm = (arms * cores) * partition
    scale = cells / norm
    stress = total / norm
    for k in range(6):
        stress_ref[k] = jnp.sum(stress[k : k + 1, :])
    kinds = [jnp.broadcast_to(t[7:8, :], (ROWS, lanes)) for t in tails]
    for i in range(depth):
        for r in range(0, near, ROWS):
            values = [shares_ref[a, i * near + r : i * near + r + ROWS, :] for a in senders]
            for kind in range(species):
                picked = [jnp.where(kinds[a] == float(kind), values[a], 0.0) for a in senders]
                result = picked[0]
                for value in picked[1:]:
                    result = result + value
                density_ref[kind, i, r : r + ROWS, :] = result * scale


def local(field_w, metric, arm_length, arm_steps, arm_species):
    species, depth, rows, lanes = field_w.shape
    arms, slabs, cores = arm_length.shape[0], lax.axis_size("slab"), lax.axis_size("arm")
    assert slabs % arms == 0 and slabs & (slabs - 1) == 0 and cores == species == 2 and rows % (2 * ROWS) == 0
    planes, parts = slabs * depth, rows // ROWS
    f32, vmem, smem = jnp.float32, pl.BlockSpec(memory_space=pltpu.VMEM), pl.BlockSpec(memory_space=pltpu.SMEM)
    size = 4 * planes * rows * lanes
    params = pltpu.CompilerParams(vmem_limit_bytes=(STEPS + 16) * size)
    small = pltpu.CompilerParams(vmem_limit_bytes=8 * size)
    swap = [(0, 1), (1, 0)]

    arguments = (arm_length, arm_steps, arm_species, metric, field_w)
    chosen, table = pl.pallas_call(
        prepare_kernel,
        out_shape=[
            jax.ShapeDtypeStruct((depth, rows, lanes), f32),
            jax.ShapeDtypeStruct((METRIC + 6, ROWS, lanes), f32),
        ],
        in_specs=[pl.BlockSpec(memory_space=pltpu.HBM)] * 5,
        out_specs=[vmem] * 2,
        scratch_shapes=[pltpu.SMEM(a.shape, a.dtype) for a in arguments[:4]]
        + [pltpu.VMEM(field_w.shape, f32), pltpu.SemaphoreType.DMA((5,))],
        compiler_params=small,
        name="prepare",
    )(*(pltpu.with_memory_space_constraint(a, pltpu.HBM) for a in arguments))
    def from_slab(value, block):
        return lax.ppermute(value, "slab", [(i, i ^ block) for i in range(slabs)])

    held = {0: chosen}
    for block in range(slabs - 2, 0, -2):
        held[block] = from_slab(chosen, block)
    for block in (0, *range(slabs - 2, 0, -2)):
        held[block + 1] = from_slab(held[block], 1)
    held = [held[block] for block in range(slabs)]
    beside = lax.ppermute(jnp.stack(held), "arm", swap)

    grid = (planes, parts, ROWS, lanes)
    piece = (planes, parts // 2, ROWS, lanes)
    hist, half, keep, give = pl.pallas_call(
        functools.partial(forward_kernel, slabs),
        out_shape=[
            jax.ShapeDtypeStruct((STEPS,) + grid, f32),
            jax.ShapeDtypeStruct(grid, f32),
            jax.ShapeDtypeStruct(piece, f32),
            jax.ShapeDtypeStruct(piece, f32),
        ],
        in_specs=[vmem] * (2 + slabs),
        out_specs=[vmem] * 4,
        scratch_shapes=[pltpu.VMEM(grid, f32)] + [pltpu.VMEM((2,) + grid, f32)] * 3,
        compiler_params=params,
        name="forward",
    )(table, beside, *held)

    other = lax.ppermute(give, "arm", swap)
    flat = (slabs, depth * (parts // 2) * ROWS, lanes)
    pairs = lax.all_to_all((keep * other).reshape(flat), "slab", 0, 0, tiled=True)
    rest = pl.pallas_call(
        functools.partial(exclusive_kernel, arms),
        out_shape=jax.ShapeDtypeStruct(flat, f32),
        in_specs=[vmem],
        out_specs=vmem,
        compiler_params=small,
        name="exclusive",
    )(pairs)
    rest = lax.all_to_all(rest, "slab", 0, 0, tiled=True).reshape(piece)
    beyond = lax.ppermute(rest * keep, "arm", swap)

    body = depth * (rows // cores)
    shares = pl.pallas_call(
        adjoint_kernel,
        out_shape=jax.ShapeDtypeStruct((slabs * cores, body + ROWS, lanes), f32),
        in_specs=[vmem] * 5,
        out_specs=vmem,
        scratch_shapes=[
            pltpu.VMEM(grid, f32),
            pltpu.VMEM(grid, f32),
            pltpu.VMEM((planes, rows, lanes), f32),
            pltpu.VMEM((ROWS, lanes), f32),
            pltpu.VMEM((6, ROWS, lanes), f32),
        ]
        + [pltpu.VMEM((2,) + grid, f32)] * 3,
        compiler_params=params,
        name="adjoint",
    )(table, hist, half, rest * other, beyond)

    shares = lax.all_to_all(shares, ("slab", "arm"), 0, 0, tiled=True)
    cells = float(planes * rows * lanes)
    return pl.pallas_call(
        functools.partial(owner_kernel, arms, cores, cells),
        out_shape=[
            jax.ShapeDtypeStruct((species, depth, rows // cores, lanes), f32),
            jax.ShapeDtypeStruct((6,), f32),
        ],
        in_specs=[vmem],
        out_specs=[vmem, smem],
        compiler_params=small,
        name="owner",
    )(shares)


def solution(mesh):
    return jax.shard_map(
        local,
        mesh=mesh,
        in_specs=(P(None, ("phase", "slab"), None, None), P("phase"), P("arm"), P("arm"), P("arm")),
        out_specs=(P(None, ("phase", "slab"), "arm", None), P("phase")),
        check_vma=False,
    )
```

```python
import functools

import jax
import jax.numpy as jnp
from jax import lax
from jax.experimental import pallas as pl
from jax.experimental.pallas import tpu as pltpu
from jax.sharding import PartitionSpec as P

STEPS = 16

ROWS = 8


def up_y(parts):
    return parts[1:] + [pltpu.roll(parts[0], ROWS - 1, 0)]


def down_y(parts):
    return [pltpu.roll(parts[-1], 1, 0)] + parts[:-1]


def up_z(value):
    return pltpu.roll(value, value.shape[1] - 1, 1)


def down_z(value):
    return pltpu.roll(value, 1, 1)


def splat(scalar, lanes):
    return jnp.full((ROWS, lanes), scalar, jnp.float32)


MU, COUNT, SPECIES, METRIC = 0, 1, 2, 3


def prepare_kernel(*refs):
    sources, (chosen_ref, table_ref), targets, sems = refs[:5], refs[5:7], refs[7:12], refs[12]
    copies = [pltpu.make_async_copy(s, t, sems.at[i]) for i, (s, t) in enumerate(zip(sources, targets))]
    for copy in copies:
        copy.start()
    for copy in copies:
        copy.wait()
    length_ref, steps_ref, species_ref, metric_ref, field_ref = targets
    arms, lanes = length_ref.shape[0], table_ref.shape[2]
    arm = lax.rem(lax.axis_index("slab"), arms)
    steps = splat(steps_ref[arm].astype(jnp.float32), lanes)
    mu = splat(length_ref[arm], lanes) / steps
    table_ref[MU] = mu
    table_ref[COUNT] = steps
    table_ref[SPECIES] = splat(species_ref[arm].astype(jnp.float32), lanes)
    for k in range(6):
        table_ref[METRIC + k] = (mu if k < 3 else 0.5 * mu) * metric_ref[k]
    chosen_ref[...] = field_ref[lax.axis_index("arm")]


def unpack(table_ref):
    count = table_ref[COUNT][0, 0].astype(jnp.int32)
    return count, table_ref[MU], [table_ref[METRIC + k] for k in range(6)]


def put(state, x, j, value):
    value_ref, sum_ref, slope_ref = state
    above, below = up_z(value), down_z(value)
    value_ref[x, j] = value
    sum_ref[x, j] = above + below
    slope_ref[x, j] = above - below


def sweep(state, visit):
    value_ref, sum_ref, slope_ref = state
    planes, parts = value_ref.shape[:2]

    def plane(ref, x):
        return [ref[x % planes, j] for j in range(parts)]

    minus, centre = plane(value_ref, -1), plane(value_ref, 0)
    slope_minus, slope = plane(slope_ref, -1), plane(slope_ref, 0)
    for x in range(planes):
        plus, slope_plus = plane(value_ref, x + 1), plane(slope_ref, x + 1)
        diff = [p - m for p, m in zip(plus, minus)]
        above, below = up_y(centre), down_y(centre)
        for j in range(parts):
            visit(
                x, j, centre[j], plus[j] + minus[j], above[j] + below[j], sum_ref[x, j], diff,
                slope_plus[j] - slope_minus[j], slope,
            )
        minus, centre = centre, plus
        slope_minus, slope = slope, slope_plus


def in_pairs(count, step, first, second):
    lone = lax.rem(count, 2)
    pl.when(lone == 1)(lambda: step(0, second, first))

    @pl.loop(0, count // 2)
    def _(pair):
        step(lone + 2 * pair, first, second)
        step(lone + 2 * pair + 1, second, first)


def forward_kernel(blocks, table_ref, other_ref, *refs):
    own_refs = refs[:blocks]
    hist_ref, half_ref, keep_ref, give_ref, gain_ref, *scratch = refs[blocks:]
    planes, parts = half_ref.shape[:2]
    depth = own_refs[0].shape[0]
    core = lax.axis_index("arm")
    count, mu, (c_x, c_y, c_z, c_xy, c_xz, c_yz) = unpack(table_ref)
    c_0 = 1.0 - 2.0 * (c_x + c_y + c_z)
    c_0, c_y, c_z, c_xy, c_xz, c_yz = (c / c_x for c in (c_0, c_y, c_z, c_xy, c_xz, c_yz))
    decay = -0.5 * mu
    start, first, second = (tuple(r.at[at] for r in scratch) for at in (lax.rem(count, 2), 0, 1))

    def begin(block_ref, block):
        base = (lax.axis_index("slab") ^ block) * depth
        for i in range(depth):
            for j in range(parts):
                half = jnp.exp(decay * block_ref[i, pl.ds(j, ROWS, stride=parts), :])
                half_ref[base + i, j] = half
                gain_ref[base + i, j] = c_x * half
                put(start, base + i, j, half)

    mine = table_ref[SPECIES][0, 0].astype(jnp.int32) == core

    @pl.when(mine)
    def _():
        for block in range(blocks):
            begin(own_refs[block], block)

    @pl.when(jnp.logical_not(mine))
    def _():
        for block in range(blocks):
            begin(other_ref.at[block], block)

    def step(k, source, target):
        def visit(x, j, centre, sum_x, sum_y, sum_z, diff, slope_x, slope):
            if j == 0:
                skew = [c_xy * d + c_yz * s for d, s in zip(diff, slope)]
                visit.skew = [a - b for a, b in zip(up_y(skew), down_y(skew))]
            value = (
                (c_0 * centre + sum_x) + (c_y * sum_y + c_z * sum_z) + (c_xz * slope_x + visit.skew[j])
            )
            value = gain_ref[x, j] * value
            hist_ref[k, x, j] = value
            put(target, x, j, half_ref[x, j] * value)

        sweep(source, visit)

    in_pairs(count, step, first, second)
    split = parts // 2
    for x in range(planes):
        for j in range(split):
            keep_ref[x, j] = hist_ref[count - 1, x, core * split + j]
            give_ref[x, j] = hist_ref[count - 1, x, (1 - core) * split + j]


def exclusive_kernel(arms, pairs_ref, out_ref):
    slabs, rows, _ = pairs_ref.shape

    @pl.loop(0, rows // ROWS)
    def _(block):
        at = pl.ds(pl.multiple_of(block * ROWS, ROWS), ROWS)
        values = [pairs_ref[a, at, :] for a in range(arms)]
        before, after = [None] * arms, [None] * arms
        for a in range(1, arms):
            before[a] = values[a - 1] if before[a - 1] is None else before[a - 1] * values[a - 1]
            b = arms - 1 - a
            after[b] = values[b + 1] if after[b + 1] is None else after[b + 1] * values[b + 1]
        for a in range(arms):
            sides = [s for s in (before[a], after[a]) if s is not None]
            result = sides[0] * sides[1] if len(sides) == 2 else sides[0]
            for copy in range(a, slabs, arms):
                out_ref[copy, at, :] = result


def adjoint_kernel(
    arms, table_ref, hist_ref, half_ref, mine_ref, other_ref, stay_ref, leave_ref, square_ref, density_ref, line_ref, tail_ref,
    total_ref, *scratch
):
    planes, parts, _, lanes = half_ref.shape
    core = lax.axis_index("arm")
    count, mu, (c_x, c_y, c_z, c_xy, c_xz, c_yz) = unpack(table_ref)
    start, first, second = (tuple(r.at[at] for r in scratch) for at in (lax.rem(count, 2), 0, 1))
    split = parts // 2
    zero = jnp.zeros((ROWS, lanes), jnp.float32)

    partition = zero
    for x in range(planes):
        for j in range(split):
            for source, side in ((mine_ref, core), (other_ref, 1 - core)):
                at = side * split + j
                adjoint = source[x, j]
                half = half_ref[x, at]
                value = half * adjoint
                end = hist_ref[count - 1, x, at]
                put(start, x, at, value)
                square_ref[x, at] = half * half
                density_ref[x, at] = (-0.5 * end) * value
                partition = partition + end * adjoint

    def step(k, source, target):
        sums = [total_ref[i] for i in range(6)]

        def visit(x, j, centre, sum_x, sum_y, sum_z, diff, slope_x, slope):
            if j == 0:
                visit.d_xy = [a - b for a, b in zip(up_y(diff), down_y(diff))]
                visit.d_yz = [a - b for a, b in zip(up_y(slope), down_y(slope))]
            twice = centre + centre
            s_xx, s_yy, s_zz = sum_x - twice, sum_y - twice, sum_z - twice
            s_xy, s_yz = visit.d_xy[j], visit.d_yz[j]
            value = (
                (centre + c_x * s_xx) + (c_y * s_yy + c_z * s_zz)
                + (c_xz * slope_x + (c_xy * s_xy + c_yz * s_yz))
            )
            put(target, x, j, square_ref[x, j] * value)
            paired = hist_ref[count - 1 - k, x, j]
            density_ref[x, j] = density_ref[x, j] + paired * centre
            for i, term in enumerate((s_xx, s_yy, s_zz, s_xy, slope_x, s_yz)):
                sums[i] = sums[i] + paired * term

        sweep(source, visit)
        for i in range(6):
            total_ref[i] = sums[i]

    for i in range(6):
        total_ref[i] = zero
    in_pairs(count, step, first, second)
    sums = [total_ref[i] for i in range(6)]

    for x in range(planes):
        for j in range(parts):
            density = density_ref[x, j] + 0.5 * first[0][x, j]
            line_ref[x, pl.ds(j, ROWS, stride=parts), :] = mu * density / half_ref[x, j]

    slab, cores = lax.axis_index("slab"), lax.axis_size("arm")
    depth, near = planes // stay_ref.shape[0], line_ref.shape[1] // cores
    kinds = (stay_ref.shape[1] - ROWS) // (depth * near)
    live = splat((slab < arms).astype(jnp.float32), lanes)
    chosen = [jnp.where(table_ref[SPECIES] == float(kind), live, 0.0) for kind in range(kinds)]
    weights = (1.0, 1.0, 1.0, 0.25, 0.25, 0.25)
    for k in range(6):
        tail_ref[k : k + 1, :] = jnp.sum((weights[k] * mu) * sums[k], axis=0, keepdims=True)
    tail_ref[6:7, :] = jnp.sum(partition, axis=0, keepdims=True)
    tail_ref[7:8, :] = jnp.zeros((1, lanes), jnp.float32)
    tail = live * tail_ref[...]

    @pl.loop(0, stay_ref.shape[0])
    def _(block):
        base = (slab ^ block) * depth
        for target_ref, side in ((stay_ref, core), (leave_ref, 1 - core)):
            for i in range(depth):
                for r in range(0, near, ROWS):
                    value = line_ref[base + i, pl.ds(pl.multiple_of(side * near + r, ROWS), ROWS), :]
                    for kind in range(kinds):
                        row = (kind * depth + i) * near + r
                        target_ref[block, row : row + ROWS, :] = chosen[kind] * value
            target_ref[block, kinds * depth * near :, :] = tail


def join_kernel(block, stay_ref, passed_ref, out_ref):
    out_ref[...] = stay_ref[block] + passed_ref[...]


def owner_kernel(cells, *refs):
    sources, (density_ref, stress_ref) = refs[:-2], refs[-2:]
    species, depth, near, lanes = density_ref.shape

    def total(row):
        values = [source[row : row + ROWS, :] for source in sources]
        while len(values) > 1:
            values = [a + b for a, b in zip(values[::2], values[1::2])]
        return values[0]

    tail = total(species * depth * near)
    norm = jnp.broadcast_to(jnp.sum(tail[6:7, :], axis=1, keepdims=True), (ROWS, lanes))
    scale = cells / norm
    stress = tail / norm
    for k in range(6):
        stress_ref[k] = jnp.sum(stress[k : k + 1, :])
    for kind in range(species):
        for i in range(depth):
            for r in range(0, near, ROWS):
                density_ref[kind, i, r : r + ROWS, :] = scale * total((kind * depth + i) * near + r)


def local(field_w, metric, arm_length, arm_steps, arm_species):
    species, depth, rows, lanes = field_w.shape
    arms, slabs, cores = arm_length.shape[0], lax.axis_size("slab"), lax.axis_size("arm")
    assert slabs % arms == 0 and slabs & (slabs - 1) == 0 and cores == species == 2 and rows % (2 * ROWS) == 0
    planes, parts = slabs * depth, rows // ROWS
    f32, vmem, smem = jnp.float32, pl.BlockSpec(memory_space=pltpu.VMEM), pl.BlockSpec(memory_space=pltpu.SMEM)
    size = 4 * planes * rows * lanes
    params = pltpu.CompilerParams(vmem_limit_bytes=(STEPS + 16) * size)
    small = pltpu.CompilerParams(vmem_limit_bytes=8 * size)
    swap = [(0, 1), (1, 0)]

    arguments = (arm_length, arm_steps, arm_species, metric, field_w)
    chosen, table = pl.pallas_call(
        prepare_kernel,
        out_shape=[
            jax.ShapeDtypeStruct((depth, rows, lanes), f32),
            jax.ShapeDtypeStruct((METRIC + 6, ROWS, lanes), f32),
        ],
        in_specs=[pl.BlockSpec(memory_space=pltpu.HBM)] * 5,
        out_specs=[vmem] * 2,
        scratch_shapes=[pltpu.SMEM(a.shape, a.dtype) for a in arguments[:4]]
        + [pltpu.VMEM(field_w.shape, f32), pltpu.SemaphoreType.DMA((5,))],
        compiler_params=small,
        name="prepare",
    )(*(pltpu.with_memory_space_constraint(a, pltpu.HBM) for a in arguments))
    def from_slab(value, block):
        return lax.ppermute(value, "slab", [(i, i ^ block) for i in range(slabs)])

    held = {0: chosen}
    for block in range(slabs - 2, 0, -2):
        held[block] = from_slab(chosen, block)
    for block in (0, *range(slabs - 2, 0, -2)):
        held[block + 1] = from_slab(held[block], 1)
    held = [held[block] for block in range(slabs)]
    beside = lax.ppermute(jnp.stack(held), "arm", swap)

    grid = (planes, parts, ROWS, lanes)
    piece = (planes, parts // 2, ROWS, lanes)
    hist, half, keep, give = pl.pallas_call(
        functools.partial(forward_kernel, slabs),
        out_shape=[
            jax.ShapeDtypeStruct((STEPS,) + grid, f32),
            jax.ShapeDtypeStruct(grid, f32),
            jax.ShapeDtypeStruct(piece, f32),
            jax.ShapeDtypeStruct(piece, f32),
        ],
        in_specs=[vmem] * (2 + slabs),
        out_specs=[vmem] * 4,
        scratch_shapes=[pltpu.VMEM(grid, f32)] + [pltpu.VMEM((2,) + grid, f32)] * 3,
        compiler_params=params,
        name="forward",
    )(table, beside, *held)

    other = lax.ppermute(give, "arm", swap)
    flat = (slabs, depth * (parts // 2) * ROWS, lanes)
    pairs = lax.all_to_all((keep * other).reshape(flat), "slab", 0, 0, tiled=True)
    rest = pl.pallas_call(
        functools.partial(exclusive_kernel, arms),
        out_shape=jax.ShapeDtypeStruct(flat, f32),
        in_specs=[vmem],
        out_specs=vmem,
        compiler_params=small,
        name="exclusive",
    )(pairs)
    rest = lax.all_to_all(rest, "slab", 0, 0, tiled=True).reshape(piece)
    beyond = lax.ppermute(rest * keep, "arm", swap)

    block = jax.ShapeDtypeStruct((slabs, species * depth * (rows // cores) + ROWS, lanes), f32)
    stay, leave = pl.pallas_call(
        functools.partial(adjoint_kernel, arms),
        out_shape=[block, block],
        in_specs=[vmem] * 5,
        out_specs=[vmem] * 2,
        scratch_shapes=[
            pltpu.VMEM(grid, f32),
            pltpu.VMEM(grid, f32),
            pltpu.VMEM((planes, rows, lanes), f32),
            pltpu.VMEM((ROWS, lanes), f32),
            pltpu.VMEM((6, ROWS, lanes), f32),
        ]
        + [pltpu.VMEM((2,) + grid, f32)] * 3,
        compiler_params=params,
        name="adjoint",
    )(table, hist, half, rest * other, beyond)

    stay = stay + lax.ppermute(leave, "arm", swap)
    passed = {block: from_slab(stay[block + 1], 1) for block in range(slabs - 2, -1, -2)}
    pairs = {
        block: pl.pallas_call(
            functools.partial(join_kernel, block),
            out_shape=jax.ShapeDtypeStruct(value.shape, f32),
            in_specs=[vmem] * 2,
            out_specs=vmem,
            compiler_params=small,
            name="join",
        )(stay, value)
        for block, value in passed.items()
    }
    sums = {0: pairs[0]}
    for block in range(slabs - 2, 0, -2):
        sums[block] = from_slab(pairs[block], block)
    return pl.pallas_call(
        functools.partial(owner_kernel, float(planes * rows * lanes)),
        out_shape=[
            jax.ShapeDtypeStruct((species, depth, rows // cores, lanes), f32),
            jax.ShapeDtypeStruct((6,), f32),
        ],
        in_specs=[vmem] * (slabs // 2),
        out_specs=[vmem, smem],
        compiler_params=small,
        name="owner",
    )(*(sums[block] for block in range(0, slabs, 2)))


def solution(mesh):
    return jax.shard_map(
        local,
        mesh=mesh,
        in_specs=(P(None, ("phase", "slab"), None, None), P("phase"), P("arm"), P("arm"), P("arm")),
        out_specs=(P(None, ("phase", "slab"), "arm", None), P("phase")),
        check_vma=False,
    )
```

```python
import functools

import jax
import jax.numpy as jnp
from jax import lax
from jax.experimental import pallas as pl
from jax.experimental.pallas import tpu as pltpu
from jax.sharding import PartitionSpec as P

STEPS = 16

ROWS = 8


def up_y(parts):
    return parts[1:] + [pltpu.roll(parts[0], ROWS - 1, 0)]


def down_y(parts):
    return [pltpu.roll(parts[-1], 1, 0)] + parts[:-1]


def up_z(value):
    return pltpu.roll(value, value.shape[1] - 1, 1)


def down_z(value):
    return pltpu.roll(value, 1, 1)


def splat(scalar, lanes):
    return jnp.full((ROWS, lanes), scalar, jnp.float32)


MU, COUNT, SPECIES, METRIC = 0, 1, 2, 3


def prepare_kernel(*refs):
    sources, (chosen_ref, table_ref), targets, sems = refs[:5], refs[5:7], refs[7:12], refs[12]
    copies = [pltpu.make_async_copy(s, t, sems.at[i]) for i, (s, t) in enumerate(zip(sources, targets))]
    for copy in copies:
        copy.start()
    for copy in copies:
        copy.wait()
    length_ref, steps_ref, species_ref, metric_ref, field_ref = targets
    arms, lanes = length_ref.shape[0], table_ref.shape[2]
    arm = lax.rem(lax.axis_index("slab"), arms)
    steps = splat(steps_ref[arm].astype(jnp.float32), lanes)
    mu = splat(length_ref[arm], lanes) / steps
    table_ref[MU] = mu
    table_ref[COUNT] = steps
    table_ref[SPECIES] = splat(species_ref[arm].astype(jnp.float32), lanes)
    for k in range(6):
        table_ref[METRIC + k] = (mu if k < 3 else 0.5 * mu) * metric_ref[k]
    chosen_ref[...] = field_ref[lax.axis_index("arm")]


def unpack(table_ref):
    count = table_ref[COUNT][0, 0].astype(jnp.int32)
    return count, table_ref[MU], [table_ref[METRIC + k] for k in range(6)]


def put(state, x, j, value):
    value_ref, sum_ref, slope_ref = state
    above, below = up_z(value), down_z(value)
    value_ref[x, j] = value
    sum_ref[x, j] = above + below
    slope_ref[x, j] = above - below


def sweep(state, visit):
    value_ref, sum_ref, slope_ref = state
    planes, parts = value_ref.shape[:2]

    def plane(ref, x):
        return [ref[x % planes, j] for j in range(parts)]

    minus, centre = plane(value_ref, -1), plane(value_ref, 0)
    slope_minus, slope = plane(slope_ref, -1), plane(slope_ref, 0)
    for x in range(planes):
        plus, slope_plus = plane(value_ref, x + 1), plane(slope_ref, x + 1)
        diff = [p - m for p, m in zip(plus, minus)]
        above, below = up_y(centre), down_y(centre)
        for j in range(parts):
            visit(
                x, j, centre[j], plus[j] + minus[j], above[j] + below[j], sum_ref[x, j], diff,
                slope_plus[j] - slope_minus[j], slope,
            )
        minus, centre = centre, plus
        slope_minus, slope = slope, slope_plus


def in_pairs(count, step, first, second):
    lone = lax.rem(count, 2)
    pl.when(lone == 1)(lambda: step(0, second, first))

    @pl.loop(0, count // 2)
    def _(pair):
        step(lone + 2 * pair, first, second)
        step(lone + 2 * pair + 1, second, first)


def forward_kernel(blocks, table_ref, other_ref, *refs):
    own_refs = refs[:blocks]
    hist_ref, half_ref, keep_ref, give_ref, gain_ref, *scratch = refs[blocks:]
    planes, parts = half_ref.shape[:2]
    depth = own_refs[0].shape[0]
    core = lax.axis_index("arm")
    count, mu, (c_x, c_y, c_z, c_xy, c_xz, c_yz) = unpack(table_ref)
    c_0 = 1.0 - 2.0 * (c_x + c_y + c_z)
    c_0, c_y, c_z, c_xy, c_xz, c_yz = (c / c_x for c in (c_0, c_y, c_z, c_xy, c_xz, c_yz))
    decay = -0.5 * mu
    start, first, second = (tuple(r.at[at] for r in scratch) for at in (lax.rem(count, 2), 0, 1))

    def begin(block_ref, block):
        base = (lax.axis_index("slab") ^ block) * depth
        for i in range(depth):
            for j in range(parts):
                half = jnp.exp(decay * block_ref[i, pl.ds(j, ROWS, stride=parts), :])
                half_ref[base + i, j] = half
                gain_ref[base + i, j] = c_x * half
                put(start, base + i, j, half)

    mine = table_ref[SPECIES][0, 0].astype(jnp.int32) == core

    @pl.when(mine)
    def _():
        for block in range(blocks):
            begin(own_refs[block], block)

    @pl.when(jnp.logical_not(mine))
    def _():
        for block in range(blocks):
            begin(other_ref.at[block], block)

    def step(k, source, target):
        def visit(x, j, centre, sum_x, sum_y, sum_z, diff, slope_x, slope):
            if j == 0:
                skew = [c_xy * d + c_yz * s for d, s in zip(diff, slope)]
                visit.skew = [a - b for a, b in zip(up_y(skew), down_y(skew))]
            value = (
                (c_0 * centre + sum_x) + (c_y * sum_y + c_z * sum_z) + (c_xz * slope_x + visit.skew[j])
            )
            value = gain_ref[x, j] * value
            hist_ref[k, x, j] = value
            put(target, x, j, half_ref[x, j] * value)

        sweep(source, visit)

    in_pairs(count, step, first, second)
    split = parts // 2
    for x in range(planes):
        for j in range(split):
            keep_ref[x, j] = hist_ref[count - 1, x, core * split + j]
            give_ref[x, j] = hist_ref[count - 1, x, (1 - core) * split + j]


def pair_kernel(arms, keep_ref, other_ref, out_ref):
    slab = lax.axis_index("slab")
    depth, parts = keep_ref.shape[0] // out_ref.shape[0], keep_ref.shape[1]

    @pl.loop(0, out_ref.shape[0])
    def _(block):
        base = (slab ^ block) * depth
        for i in range(depth):
            for j in range(parts):
                row = (i * parts + j) * ROWS
                value = keep_ref[base + i, j] * other_ref[base + i, j]
                out_ref[block, row : row + ROWS, :] = jnp.where(slab < arms, value, 1.0)


def times_kernel(block, stay_ref, passed_ref, out_ref):
    out_ref[...] = stay_ref[block] * passed_ref[...]


def exclusive_kernel(*refs):
    count = len(refs) // 2
    sources, targets = refs[:count], refs[count:]
    for row in range(0, sources[0].shape[0], ROWS):
        values = [source[row : row + ROWS, :] for source in sources]
        before, after = [None] * count, [None] * count
        for a in range(1, count):
            before[a] = values[a - 1] if before[a - 1] is None else before[a - 1] * values[a - 1]
            b = count - 1 - a
            after[b] = values[b + 1] if after[b + 1] is None else after[b + 1] * values[b + 1]
        for a in range(count):
            sides = [s for s in (before[a], after[a]) if s is not None]
            targets[a][row : row + ROWS, :] = sides[0] * sides[1] if len(sides) == 2 else sides[0]


def turn_kernel(block, back_ref, stay_ref, passed_ref, rest_ref, beside_ref):
    rest_ref[...] = back_ref[...] * passed_ref[...]
    beside_ref[...] = back_ref[...] * stay_ref[block]


def spread_kernel(keep_ref, other_ref, *refs):
    rests, (mine_ref, theirs_ref) = refs[:-2], refs[-2:]
    slab = lax.axis_index("slab")
    depth, parts = keep_ref.shape[0] // len(rests), keep_ref.shape[1]
    for block, rest_ref in enumerate(rests):
        base = (slab ^ block) * depth
        for i in range(depth):
            for j in range(parts):
                row = (i * parts + j) * ROWS
                rest = rest_ref[row : row + ROWS, :]
                mine_ref[base + i, j] = rest * other_ref[base + i, j]
                theirs_ref[base + i, j] = rest * keep_ref[base + i, j]


def adjoint_kernel(
    arms, table_ref, hist_ref, half_ref, mine_ref, other_ref, stay_ref, leave_ref, square_ref, density_ref, line_ref, tail_ref,
    total_ref, *scratch
):
    planes, parts, _, lanes = half_ref.shape
    core = lax.axis_index("arm")
    count, mu, (c_x, c_y, c_z, c_xy, c_xz, c_yz) = unpack(table_ref)
    start, first, second = (tuple(r.at[at] for r in scratch) for at in (lax.rem(count, 2), 0, 1))
    split = parts // 2
    zero = jnp.zeros((ROWS, lanes), jnp.float32)

    partition = zero
    for x in range(planes):
        for j in range(split):
            for source, side in ((mine_ref, core), (other_ref, 1 - core)):
                at = side * split + j
                adjoint = source[x, j]
                half = half_ref[x, at]
                value = half * adjoint
                end = hist_ref[count - 1, x, at]
                put(start, x, at, value)
                square_ref[x, at] = half * half
                density_ref[x, at] = (-0.5 * end) * value
                partition = partition + end * adjoint

    def step(k, source, target):
        sums = [total_ref[i] for i in range(6)]

        def visit(x, j, centre, sum_x, sum_y, sum_z, diff, slope_x, slope):
            if j == 0:
                visit.d_xy = [a - b for a, b in zip(up_y(diff), down_y(diff))]
                visit.d_yz = [a - b for a, b in zip(up_y(slope), down_y(slope))]
            twice = centre + centre
            s_xx, s_yy, s_zz = sum_x - twice, sum_y - twice, sum_z - twice
            s_xy, s_yz = visit.d_xy[j], visit.d_yz[j]
            value = (
                (centre + c_x * s_xx) + (c_y * s_yy + c_z * s_zz)
                + (c_xz * slope_x + (c_xy * s_xy + c_yz * s_yz))
            )
            put(target, x, j, square_ref[x, j] * value)
            paired = hist_ref[count - 1 - k, x, j]
            density_ref[x, j] = density_ref[x, j] + paired * centre
            for i, term in enumerate((s_xx, s_yy, s_zz, s_xy, slope_x, s_yz)):
                sums[i] = sums[i] + paired * term

        sweep(source, visit)
        for i in range(6):
            total_ref[i] = sums[i]

    for i in range(6):
        total_ref[i] = zero
    in_pairs(count, step, first, second)
    sums = [total_ref[i] for i in range(6)]

    for x in range(planes):
        for j in range(parts):
            density = density_ref[x, j] + 0.5 * first[0][x, j]
            line_ref[x, pl.ds(j, ROWS, stride=parts), :] = mu * density / half_ref[x, j]

    slab, cores = lax.axis_index("slab"), lax.axis_size("arm")
    depth, near = planes // stay_ref.shape[0], line_ref.shape[1] // cores
    kinds = (stay_ref.shape[1] - ROWS) // (depth * near)
    live = splat((slab < arms).astype(jnp.float32), lanes)
    chosen = [jnp.where(table_ref[SPECIES] == float(kind), live, 0.0) for kind in range(kinds)]
    weights = (1.0, 1.0, 1.0, 0.25, 0.25, 0.25)
    for k in range(6):
        tail_ref[k : k + 1, :] = jnp.sum((weights[k] * mu) * sums[k], axis=0, keepdims=True)
    tail_ref[6:7, :] = jnp.sum(partition, axis=0, keepdims=True)
    tail_ref[7:8, :] = jnp.zeros((1, lanes), jnp.float32)
    tail = live * tail_ref[...]

    @pl.loop(0, stay_ref.shape[0])
    def _(block):
        base = (slab ^ block) * depth
        for target_ref, side in ((stay_ref, core), (leave_ref, 1 - core)):
            for i in range(depth):
                for r in range(0, near, ROWS):
                    value = line_ref[base + i, pl.ds(pl.multiple_of(side * near + r, ROWS), ROWS), :]
                    for kind in range(kinds):
                        row = (kind * depth + i) * near + r
                        target_ref[block, row : row + ROWS, :] = chosen[kind] * value
            target_ref[block, kinds * depth * near :, :] = tail


def join_kernel(block, stay_ref, passed_ref, out_ref):
    out_ref[...] = stay_ref[block] + passed_ref[...]


def owner_kernel(cells, *refs):
    sources, (density_ref, stress_ref) = refs[:-2], refs[-2:]
    species, depth, near, lanes = density_ref.shape

    def total(row):
        values = [source[row : row + ROWS, :] for source in sources]
        while len(values) > 1:
            values = [a + b for a, b in zip(values[::2], values[1::2])]
        return values[0]

    tail = total(species * depth * near)
    norm = jnp.broadcast_to(jnp.sum(tail[6:7, :], axis=1, keepdims=True), (ROWS, lanes))
    scale = cells / norm
    stress = tail / norm
    for k in range(6):
        stress_ref[k] = jnp.sum(stress[k : k + 1, :])
    for kind in range(species):
        for i in range(depth):
            for r in range(0, near, ROWS):
                density_ref[kind, i, r : r + ROWS, :] = scale * total((kind * depth + i) * near + r)


def local(field_w, metric, arm_length, arm_steps, arm_species):
    species, depth, rows, lanes = field_w.shape
    arms, slabs, cores = arm_length.shape[0], lax.axis_size("slab"), lax.axis_size("arm")
    assert slabs % arms == 0 and slabs & (slabs - 1) == 0 and cores == species == 2 and rows % (2 * ROWS) == 0
    planes, parts = slabs * depth, rows // ROWS
    f32, vmem, smem = jnp.float32, pl.BlockSpec(memory_space=pltpu.VMEM), pl.BlockSpec(memory_space=pltpu.SMEM)
    size = 4 * planes * rows * lanes
    params = pltpu.CompilerParams(vmem_limit_bytes=(STEPS + 16) * size)
    small = pltpu.CompilerParams(vmem_limit_bytes=8 * size)
    swap = [(0, 1), (1, 0)]

    arguments = (arm_length, arm_steps, arm_species, metric, field_w)
    chosen, table = pl.pallas_call(
        prepare_kernel,
        out_shape=[
            jax.ShapeDtypeStruct((depth, rows, lanes), f32),
            jax.ShapeDtypeStruct((METRIC + 6, ROWS, lanes), f32),
        ],
        in_specs=[pl.BlockSpec(memory_space=pltpu.HBM)] * 5,
        out_specs=[vmem] * 2,
        scratch_shapes=[pltpu.SMEM(a.shape, a.dtype) for a in arguments[:4]]
        + [pltpu.VMEM(field_w.shape, f32), pltpu.SemaphoreType.DMA((5,))],
        compiler_params=small,
        name="prepare",
    )(*(pltpu.with_memory_space_constraint(a, pltpu.HBM) for a in arguments))
    def from_slab(value, block):
        return lax.ppermute(value, "slab", [(i, i ^ block) for i in range(slabs)])

    held = {0: chosen}
    for block in range(slabs - 2, 0, -2):
        held[block] = from_slab(chosen, block)
    for block in (0, *range(slabs - 2, 0, -2)):
        held[block + 1] = from_slab(held[block], 1)
    held = [held[block] for block in range(slabs)]
    beside = lax.ppermute(jnp.stack(held), "arm", swap)

    grid = (planes, parts, ROWS, lanes)
    piece = (planes, parts // 2, ROWS, lanes)
    hist, half, keep, give = pl.pallas_call(
        functools.partial(forward_kernel, slabs),
        out_shape=[
            jax.ShapeDtypeStruct((STEPS,) + grid, f32),
            jax.ShapeDtypeStruct(grid, f32),
            jax.ShapeDtypeStruct(piece, f32),
            jax.ShapeDtypeStruct(piece, f32),
        ],
        in_specs=[vmem] * (2 + slabs),
        out_specs=[vmem] * 4,
        scratch_shapes=[pltpu.VMEM(grid, f32)] + [pltpu.VMEM((2,) + grid, f32)] * 3,
        compiler_params=params,
        name="forward",
    )(table, beside, *held)

    other = lax.ppermute(give, "arm", swap)
    def call(kernel, name, outs, *args):
        return pl.pallas_call(
            kernel,
            out_shape=[jax.ShapeDtypeStruct(shape, f32) for shape in outs],
            in_specs=[vmem] * len(args),
            out_specs=[vmem] * len(outs),
            compiler_params=small,
            name=name,
        )(*args)

    flat = (depth * (parts // 2) * ROWS, lanes)
    even = range(slabs - 2, -1, -2)
    (product,) = call(functools.partial(pair_kernel, arms), "pair", [(slabs,) + flat], keep, other)
    passed = {block: from_slab(product[block + 1], 1) for block in even}
    back = {}
    for block in even:
        (value,) = call(functools.partial(times_kernel, block), "times", [flat], product, passed[block])
        back[block] = from_slab(value, block) if block else value
    order = range(0, slabs, 2)
    back = dict(zip(order, call(exclusive_kernel, "exclusive", [flat] * (slabs // 2), *(back[k] for k in order))))
    back = {block: from_slab(back[block], block) if block else back[block] for block in even}
    rests = {}
    for block in (0, *range(slabs - 2, 0, -2)):
        turn = functools.partial(turn_kernel, block)
        rests[block], value = call(turn, "turn", [flat] * 2, back[block], product, passed[block])
        rests[block + 1] = from_slab(value, 1)
    mine, theirs = call(spread_kernel, "spread", [piece] * 2, keep, other, *(rests[k] for k in range(slabs)))
    beyond = lax.ppermute(theirs, "arm", swap)

    block = jax.ShapeDtypeStruct((slabs, species * depth * (rows // cores) + ROWS, lanes), f32)
    stay, leave = pl.pallas_call(
        functools.partial(adjoint_kernel, arms),
        out_shape=[block, block],
        in_specs=[vmem] * 5,
        out_specs=[vmem] * 2,
        scratch_shapes=[
            pltpu.VMEM(grid, f32),
            pltpu.VMEM(grid, f32),
            pltpu.VMEM((planes, rows, lanes), f32),
            pltpu.VMEM((ROWS, lanes), f32),
            pltpu.VMEM((6, ROWS, lanes), f32),
        ]
        + [pltpu.VMEM((2,) + grid, f32)] * 3,
        compiler_params=params,
        name="adjoint",
    )(table, hist, half, mine, beyond)

    stay = stay + lax.ppermute(leave, "arm", swap)
    passed = {block: from_slab(stay[block + 1], 1) for block in range(slabs - 2, -1, -2)}
    pairs = {
        block: pl.pallas_call(
            functools.partial(join_kernel, block),
            out_shape=jax.ShapeDtypeStruct(value.shape, f32),
            in_specs=[vmem] * 2,
            out_specs=vmem,
            compiler_params=small,
            name="join",
        )(stay, value)
        for block, value in passed.items()
    }
    sums = {0: pairs[0]}
    for block in range(slabs - 2, 0, -2):
        sums[block] = from_slab(pairs[block], block)
    return pl.pallas_call(
        functools.partial(owner_kernel, float(planes * rows * lanes)),
        out_shape=[
            jax.ShapeDtypeStruct((species, depth, rows // cores, lanes), f32),
            jax.ShapeDtypeStruct((6,), f32),
        ],
        in_specs=[vmem] * (slabs // 2),
        out_specs=[vmem, smem],
        compiler_params=small,
        name="owner",
    )(*(sums[block] for block in range(0, slabs, 2)))


def solution(mesh):
    return jax.shard_map(
        local,
        mesh=mesh,
        in_specs=(P(None, ("phase", "slab"), None, None), P("phase"), P("arm"), P("arm"), P("arm")),
        out_specs=(P(None, ("phase", "slab"), "arm", None), P("phase")),
        check_vma=False,
    )
```

```python
import functools

import jax
import jax.numpy as jnp
from jax import lax
from jax.experimental import pallas as pl
from jax.experimental.pallas import tpu as pltpu
from jax.sharding import PartitionSpec as P

STEPS = 16

ROWS = 8


def up_y(parts):
    return parts[1:] + [pltpu.roll(parts[0], ROWS - 1, 0)]


def down_y(parts):
    return [pltpu.roll(parts[-1], 1, 0)] + parts[:-1]


def up_z(value):
    return pltpu.roll(value, value.shape[1] - 1, 1)


def down_z(value):
    return pltpu.roll(value, 1, 1)


def splat(scalar, lanes):
    return jnp.full((ROWS, lanes), scalar, jnp.float32)


MU, COUNT, SPECIES, METRIC = 0, 1, 2, 3


def prepare_kernel(*refs):
    sources, (chosen_ref, table_ref), targets, sems = refs[:5], refs[5:7], refs[7:12], refs[12]
    copies = [pltpu.make_async_copy(s, t, sems.at[i]) for i, (s, t) in enumerate(zip(sources, targets))]
    for copy in copies:
        copy.start()
    for copy in copies:
        copy.wait()
    length_ref, steps_ref, species_ref, metric_ref, field_ref = targets
    arms, lanes = length_ref.shape[0], table_ref.shape[2]
    arm = lax.rem(lax.axis_index("slab"), arms)
    steps = splat(steps_ref[arm].astype(jnp.float32), lanes)
    mu = splat(length_ref[arm], lanes) / steps
    table_ref[MU] = mu
    table_ref[COUNT] = steps
    table_ref[SPECIES] = splat(species_ref[arm].astype(jnp.float32), lanes)
    for k in range(6):
        table_ref[METRIC + k] = (mu if k < 3 else 0.5 * mu) * metric_ref[k]
    chosen_ref[...] = field_ref[lax.axis_index("arm")]


def unpack(table_ref):
    count = table_ref[COUNT][0, 0].astype(jnp.int32)
    return count, table_ref[MU], [table_ref[METRIC + k] for k in range(6)]


def put(state, x, j, value):
    value_ref, sum_ref, slope_ref = state
    above, below = up_z(value), down_z(value)
    value_ref[x, j] = value
    sum_ref[x, j] = above + below
    slope_ref[x, j] = above - below


def sweep(state, visit):
    value_ref, sum_ref, slope_ref = state
    planes, parts = value_ref.shape[:2]

    def plane(ref, x):
        return [ref[x % planes, j] for j in range(parts)]

    minus, centre = plane(value_ref, -1), plane(value_ref, 0)
    slope_minus, slope = plane(slope_ref, -1), plane(slope_ref, 0)
    for x in range(planes):
        plus, slope_plus = plane(value_ref, x + 1), plane(slope_ref, x + 1)
        diff = [p - m for p, m in zip(plus, minus)]
        above, below = up_y(centre), down_y(centre)
        for j in range(parts):
            visit(
                x, j, centre[j], plus[j] + minus[j], above[j] + below[j], sum_ref[x, j], diff,
                slope_plus[j] - slope_minus[j], slope,
            )
        minus, centre = centre, plus
        slope_minus, slope = slope, slope_plus


def in_pairs(count, step, first, second):
    lone = lax.rem(count, 2)
    pl.when(lone == 1)(lambda: step(0, second, first))

    @pl.loop(0, count // 2)
    def _(pair):
        step(lone + 2 * pair, first, second)
        step(lone + 2 * pair + 1, second, first)


def forward_kernel(blocks, table_ref, other_ref, *refs):
    own_refs = refs[:blocks]
    hist_ref, half_ref, keep_ref, give_ref, gain_ref, *scratch = refs[blocks:]
    planes, parts = half_ref.shape[:2]
    depth = own_refs[0].shape[0]
    core = lax.axis_index("arm")
    count, mu, (c_x, c_y, c_z, c_xy, c_xz, c_yz) = unpack(table_ref)
    c_0 = 1.0 - 2.0 * (c_x + c_y + c_z)
    c_0, c_y, c_z, c_xy, c_xz, c_yz = (c / c_x for c in (c_0, c_y, c_z, c_xy, c_xz, c_yz))
    decay = -0.5 * mu
    start, first, second = (tuple(r.at[at] for r in scratch) for at in (lax.rem(count, 2), 0, 1))

    def begin(block_ref, block):
        base = (lax.axis_index("slab") ^ block) * depth
        for i in range(depth):
            for j in range(parts):
                half = jnp.exp(decay * block_ref[i, pl.ds(j, ROWS, stride=parts), :])
                half_ref[base + i, j] = half
                gain_ref[base + i, j] = c_x * half
                put(start, base + i, j, half)

    mine = table_ref[SPECIES][0, 0].astype(jnp.int32) == core

    @pl.when(mine)
    def _():
        for block in range(blocks):
            begin(own_refs[block], block)

    @pl.when(jnp.logical_not(mine))
    def _():
        for block in range(blocks):
            begin(other_ref.at[block], block)

    def step(k, source, target):
        def visit(x, j, centre, sum_x, sum_y, sum_z, diff, slope_x, slope):
            if j == 0:
                skew = [c_xy * d + c_yz * s for d, s in zip(diff, slope)]
                visit.skew = [a - b for a, b in zip(up_y(skew), down_y(skew))]
            value = (
                (c_0 * centre + sum_x) + (c_y * sum_y + c_z * sum_z) + (c_xz * slope_x + visit.skew[j])
            )
            value = gain_ref[x, j] * value
            hist_ref[k, x, j] = value
            put(target, x, j, half_ref[x, j] * value)

        sweep(source, visit)

    in_pairs(count, step, first, second)
    split = parts // 2
    for x in range(planes):
        for j in range(split):
            keep_ref[x, j] = hist_ref[count - 1, x, core * split + j]
            give_ref[x, j] = hist_ref[count - 1, x, (1 - core) * split + j]


def pair_kernel(arms, keep_ref, other_ref, out_ref):
    slab = lax.axis_index("slab")
    depth, parts = keep_ref.shape[0] // out_ref.shape[0], keep_ref.shape[1]

    @pl.loop(0, out_ref.shape[0])
    def _(block):
        base = (slab ^ block) * depth
        for i in range(depth):
            for j in range(parts):
                row = (i * parts + j) * ROWS
                value = keep_ref[base + i, j] * other_ref[base + i, j]
                out_ref[block, row : row + ROWS, :] = jnp.where(slab < arms, value, 1.0)


def times_kernel(block, stay_ref, passed_ref, out_ref):
    out_ref[...] = stay_ref[block] * passed_ref[block // 2]


def exclusive_kernel(*refs):
    count = len(refs) // 2
    sources, targets = refs[:count], refs[count:]
    for row in range(0, sources[0].shape[0], ROWS):
        values = [source[row : row + ROWS, :] for source in sources]
        before, after = [None] * count, [None] * count
        for a in range(1, count):
            before[a] = values[a - 1] if before[a - 1] is None else before[a - 1] * values[a - 1]
            b = count - 1 - a
            after[b] = values[b + 1] if after[b + 1] is None else after[b + 1] * values[b + 1]
        for a in range(count):
            sides = [s for s in (before[a], after[a]) if s is not None]
            targets[a][row : row + ROWS, :] = sides[0] * sides[1] if len(sides) == 2 else sides[0]


def turn_kernel(block, back_ref, stay_ref, passed_ref, rest_ref, beside_ref):
    rest_ref[...] = back_ref[...] * passed_ref[block // 2]
    beside_ref[...] = back_ref[...] * stay_ref[block]


def spread_kernel(keep_ref, other_ref, *refs):
    rests, (mine_ref, theirs_ref) = refs[:-2], refs[-2:]
    slab = lax.axis_index("slab")
    depth, parts = keep_ref.shape[0] // len(rests), keep_ref.shape[1]
    for block, rest_ref in enumerate(rests):
        base = (slab ^ block) * depth
        for i in range(depth):
            for j in range(parts):
                row = (i * parts + j) * ROWS
                rest = rest_ref[row : row + ROWS, :]
                mine_ref[base + i, j] = rest * other_ref[base + i, j]
                theirs_ref[base + i, j] = rest * keep_ref[base + i, j]


def adjoint_kernel(
    arms, table_ref, hist_ref, half_ref, mine_ref, other_ref, stay_ref, leave_ref, square_ref, density_ref, line_ref, tail_ref,
    total_ref, *scratch
):
    planes, parts, _, lanes = half_ref.shape
    core = lax.axis_index("arm")
    count, mu, (c_x, c_y, c_z, c_xy, c_xz, c_yz) = unpack(table_ref)
    start, first, second = (tuple(r.at[at] for r in scratch) for at in (lax.rem(count, 2), 0, 1))
    split = parts // 2
    zero = jnp.zeros((ROWS, lanes), jnp.float32)

    partition = zero
    for x in range(planes):
        for j in range(split):
            for source, side in ((mine_ref, core), (other_ref, 1 - core)):
                at = side * split + j
                adjoint = source[x, j]
                half = half_ref[x, at]
                value = half * adjoint
                end = hist_ref[count - 1, x, at]
                put(start, x, at, value)
                square_ref[x, at] = half * half
                density_ref[x, at] = (-0.5 * end) * value
                partition = partition + end * adjoint

    def step(k, source, target):
        sums = [total_ref[i] for i in range(6)]

        def visit(x, j, centre, sum_x, sum_y, sum_z, diff, slope_x, slope):
            if j == 0:
                visit.d_xy = [a - b for a, b in zip(up_y(diff), down_y(diff))]
                visit.d_yz = [a - b for a, b in zip(up_y(slope), down_y(slope))]
            twice = centre + centre
            s_xx, s_yy, s_zz = sum_x - twice, sum_y - twice, sum_z - twice
            s_xy, s_yz = visit.d_xy[j], visit.d_yz[j]
            value = (
                (centre + c_x * s_xx) + (c_y * s_yy + c_z * s_zz)
                + (c_xz * slope_x + (c_xy * s_xy + c_yz * s_yz))
            )
            put(target, x, j, square_ref[x, j] * value)
            paired = hist_ref[count - 1 - k, x, j]
            density_ref[x, j] = density_ref[x, j] + paired * centre
            for i, term in enumerate((s_xx, s_yy, s_zz, s_xy, slope_x, s_yz)):
                sums[i] = sums[i] + paired * term

        sweep(source, visit)
        for i in range(6):
            total_ref[i] = sums[i]

    for i in range(6):
        total_ref[i] = zero
    in_pairs(count, step, first, second)
    sums = [total_ref[i] for i in range(6)]

    for x in range(planes):
        for j in range(parts):
            density = density_ref[x, j] + 0.5 * first[0][x, j]
            line_ref[x, pl.ds(j, ROWS, stride=parts), :] = mu * density / half_ref[x, j]

    slab, cores = lax.axis_index("slab"), lax.axis_size("arm")
    depth, near = planes // stay_ref.shape[0], line_ref.shape[1] // cores
    kinds = (stay_ref.shape[1] - ROWS) // (depth * near)
    live = splat((slab < arms).astype(jnp.float32), lanes)
    chosen = [jnp.where(table_ref[SPECIES] == float(kind), live, 0.0) for kind in range(kinds)]
    weights = (1.0, 1.0, 1.0, 0.25, 0.25, 0.25)
    for k in range(6):
        tail_ref[k : k + 1, :] = jnp.sum((weights[k] * mu) * sums[k], axis=0, keepdims=True)
    tail_ref[6:7, :] = jnp.sum(partition, axis=0, keepdims=True)
    tail_ref[7:8, :] = jnp.zeros((1, lanes), jnp.float32)
    tail = live * tail_ref[...]

    @pl.loop(0, stay_ref.shape[0])
    def _(block):
        base = (slab ^ block) * depth
        for target_ref, side in ((stay_ref, core), (leave_ref, 1 - core)):
            for i in range(depth):
                for r in range(0, near, ROWS):
                    value = line_ref[base + i, pl.ds(pl.multiple_of(side * near + r, ROWS), ROWS), :]
                    for kind in range(kinds):
                        row = (kind * depth + i) * near + r
                        target_ref[block, row : row + ROWS, :] = chosen[kind] * value
            target_ref[block, kinds * depth * near :, :] = tail


def join_kernel(block, stay_ref, passed_ref, out_ref):
    out_ref[...] = stay_ref[block] + passed_ref[...]


def owner_kernel(cells, *refs):
    sources, (density_ref, stress_ref) = refs[:-2], refs[-2:]
    species, depth, near, lanes = density_ref.shape

    def total(row):
        values = [source[row : row + ROWS, :] for source in sources]
        while len(values) > 1:
            values = [a + b for a, b in zip(values[::2], values[1::2])]
        return values[0]

    tail = total(species * depth * near)
    norm = jnp.broadcast_to(jnp.sum(tail[6:7, :], axis=1, keepdims=True), (ROWS, lanes))
    scale = cells / norm
    stress = tail / norm
    for k in range(6):
        stress_ref[k] = jnp.sum(stress[k : k + 1, :])
    for kind in range(species):
        for i in range(depth):
            for r in range(0, near, ROWS):
                density_ref[kind, i, r : r + ROWS, :] = scale * total((kind * depth + i) * near + r)


def local(field_w, metric, arm_length, arm_steps, arm_species):
    species, depth, rows, lanes = field_w.shape
    arms, slabs, cores = arm_length.shape[0], lax.axis_size("slab"), lax.axis_size("arm")
    assert slabs % arms == 0 and slabs & (slabs - 1) == 0 and cores == species == 2 and rows % (2 * ROWS) == 0
    planes, parts = slabs * depth, rows // ROWS
    f32, vmem, smem = jnp.float32, pl.BlockSpec(memory_space=pltpu.VMEM), pl.BlockSpec(memory_space=pltpu.SMEM)
    size = 4 * planes * rows * lanes
    params = pltpu.CompilerParams(vmem_limit_bytes=(STEPS + 16) * size)
    small = pltpu.CompilerParams(vmem_limit_bytes=8 * size)
    swap = [(0, 1), (1, 0)]

    arguments = (arm_length, arm_steps, arm_species, metric, field_w)
    chosen, table = pl.pallas_call(
        prepare_kernel,
        out_shape=[
            jax.ShapeDtypeStruct((depth, rows, lanes), f32),
            jax.ShapeDtypeStruct((METRIC + 6, ROWS, lanes), f32),
        ],
        in_specs=[pl.BlockSpec(memory_space=pltpu.HBM)] * 5,
        out_specs=[vmem] * 2,
        scratch_shapes=[pltpu.SMEM(a.shape, a.dtype) for a in arguments[:4]]
        + [pltpu.VMEM(field_w.shape, f32), pltpu.SemaphoreType.DMA((5,))],
        compiler_params=small,
        name="prepare",
    )(*(pltpu.with_memory_space_constraint(a, pltpu.HBM) for a in arguments))
    def from_slab(value, block):
        return lax.ppermute(value, "slab", [(i, i ^ block) for i in range(slabs)])

    held = {0: chosen}
    for block in range(slabs - 2, 0, -2):
        held[block] = from_slab(chosen, block)
    for block in (0, *range(slabs - 2, 0, -2)):
        held[block + 1] = from_slab(held[block], 1)
    held = [held[block] for block in range(slabs)]
    beside = lax.ppermute(jnp.stack(held), "arm", swap)

    grid = (planes, parts, ROWS, lanes)
    piece = (planes, parts // 2, ROWS, lanes)
    hist, half, keep, give = pl.pallas_call(
        functools.partial(forward_kernel, slabs),
        out_shape=[
            jax.ShapeDtypeStruct((STEPS,) + grid, f32),
            jax.ShapeDtypeStruct(grid, f32),
            jax.ShapeDtypeStruct(piece, f32),
            jax.ShapeDtypeStruct(piece, f32),
        ],
        in_specs=[vmem] * (2 + slabs),
        out_specs=[vmem] * 4,
        scratch_shapes=[pltpu.VMEM(grid, f32)] + [pltpu.VMEM((2,) + grid, f32)] * 3,
        compiler_params=params,
        name="forward",
    )(table, beside, *held)

    other = lax.ppermute(give, "arm", swap)
    def call(kernel, name, outs, *args):
        return pl.pallas_call(
            kernel,
            out_shape=[jax.ShapeDtypeStruct(shape, f32) for shape in outs],
            in_specs=[vmem] * len(args),
            out_specs=[vmem] * len(outs),
            compiler_params=small,
            name=name,
        )(*args)

    flat = (depth * (parts // 2) * ROWS, lanes)
    even = range(slabs - 2, -1, -2)
    (product,) = call(functools.partial(pair_kernel, arms), "pair", [(slabs,) + flat], keep, other)
    passed = from_slab(product[1::2], 1)
    back = {}
    for block in even:
        (value,) = call(functools.partial(times_kernel, block), "times", [flat], product, passed)
        back[block] = from_slab(value, block) if block else value
    order = range(0, slabs, 2)
    back = dict(zip(order, call(exclusive_kernel, "exclusive", [flat] * (slabs // 2), *(back[k] for k in order))))
    back = {block: from_slab(back[block], block) if block else back[block] for block in even}
    rests = {}
    for block in (0, *range(slabs - 2, 0, -2)):
        turn = functools.partial(turn_kernel, block)
        rests[block], value = call(turn, "turn", [flat] * 2, back[block], product, passed)
        rests[block + 1] = from_slab(value, 1)
    mine, theirs = call(spread_kernel, "spread", [piece] * 2, keep, other, *(rests[k] for k in range(slabs)))
    beyond = lax.ppermute(theirs, "arm", swap)

    block = jax.ShapeDtypeStruct((slabs, species * depth * (rows // cores) + ROWS, lanes), f32)
    stay, leave = pl.pallas_call(
        functools.partial(adjoint_kernel, arms),
        out_shape=[block, block],
        in_specs=[vmem] * 5,
        out_specs=[vmem] * 2,
        scratch_shapes=[
            pltpu.VMEM(grid, f32),
            pltpu.VMEM(grid, f32),
            pltpu.VMEM((planes, rows, lanes), f32),
            pltpu.VMEM((ROWS, lanes), f32),
            pltpu.VMEM((6, ROWS, lanes), f32),
        ]
        + [pltpu.VMEM((2,) + grid, f32)] * 3,
        compiler_params=params,
        name="adjoint",
    )(table, hist, half, mine, beyond)

    stay = stay + lax.ppermute(leave, "arm", swap)
    passed = {block: from_slab(stay[block + 1], 1) for block in range(slabs - 2, -1, -2)}
    pairs = {
        block: pl.pallas_call(
            functools.partial(join_kernel, block),
            out_shape=jax.ShapeDtypeStruct(value.shape, f32),
            in_specs=[vmem] * 2,
            out_specs=vmem,
            compiler_params=small,
            name="join",
        )(stay, value)
        for block, value in passed.items()
    }
    sums = {0: pairs[0]}
    for block in range(slabs - 2, 0, -2):
        sums[block] = from_slab(pairs[block], block)
    return pl.pallas_call(
        functools.partial(owner_kernel, float(planes * rows * lanes)),
        out_shape=[
            jax.ShapeDtypeStruct((species, depth, rows // cores, lanes), f32),
            jax.ShapeDtypeStruct((6,), f32),
        ],
        in_specs=[vmem] * (slabs // 2),
        out_specs=[vmem, smem],
        compiler_params=small,
        name="owner",
    )(*(sums[block] for block in range(0, slabs, 2)))


def solution(mesh):
    return jax.shard_map(
        local,
        mesh=mesh,
        in_specs=(P(None, ("phase", "slab"), None, None), P("phase"), P("arm"), P("arm"), P("arm")),
        out_specs=(P(None, ("phase", "slab"), "arm", None), P("phase")),
        check_vma=False,
    )
```
